256 devices in a mesh: ta: 4 (over x), ha: 8 (over z_hi, core), wa: 8 (over z_lo, y).
Axes of the slice: x: 4, y: 4, z: 8 (z_hi: 4, z_lo: 2; z = z_hi * 2 + z_lo), core: 2. Of those that a mesh axis runs over, the one named last changes fastest.
Arguments:
- tokens: bfloat16 [1, 16, 64, 64, 1024], P(None, 'ta', 'ha', 'wa'), may hold values from -40 to 40
- norm_gain: float32 [4, 1024], replicated, may hold values from 0.25 to 1.75
- qkv_weight: bfloat16 [3, 1024, 3, 1024], P(None, None, None, 'ta'), may hold values from -0.1875 to 0.1875
- qk_gain: float32 [3, 2, 64], replicated, may hold values from 0.25 to 1.75
- out_weight: bfloat16 [3, 1024, 1024], P(None, 'ta'), may hold values from -0.1875 to 0.1875
- ffn_in: bfloat16 [1024, 2, 2048], P(None, None, 'ta'), may hold values from -0.1875 to 0.1875
- ffn_out: bfloat16 [2048, 1024], P('ta'), may hold values from -0.125 to 0.125
Outputs:
- layer_out: bfloat16 [1, 16, 64, 64, 1024], P(None, 'ta', 'ha', 'wa')
The draws below stay inside these ranges and needn't reach their ends.
All inputs are finite; a program needn't handle non-finite values.
Results may differ from the reference program's by a relative error of at most 0.015.
Values may be sent and summed in bfloat16 or wider, within the bound.
A program may use at most 192 MiB of HBM per device.

```python
import math
import jax
import jax.numpy as jnp
from jax import lax

D = 1024
HEAD_DIM = 64
FF = 2048
CLIPS = 1
ATTN_WIDTH = 1024
FRAMES = 16
HEIGHT = 64
WIDTH = 64
N_TA = 4


def draw_tokens(key, part):
    key_entries, key_column, key_row = jax.random.split(key, 3)
    extent = (CLIPS, FRAMES, HEIGHT, WIDTH, D)
    entries = jnp.clip(jax.random.normal(key_entries, extent, jnp.float32), -4.0, 4.0)
    column_scale = jnp.exp(jax.random.uniform(key_column, (D,), jnp.float32, math.log(0.3), math.log(3.0)))
    row_scale = jnp.exp(jax.random.uniform(key_row, extent[:4] + (1,), jnp.float32, math.log(0.5), math.log(2.0)))
    return (entries * column_scale * row_scale).astype(jnp.bfloat16)


def levels(key, shape, cuts, least, high):
    loudness, own = 1.0, jax.random.fold_in(key, 6)
    for axis_at, blocks in cuts:
        heights = jnp.exp(jax.random.uniform(jax.random.fold_in(own, axis_at), (blocks,), jnp.float32, least / len(cuts), high / len(cuts)))
        loudness = loudness * jnp.repeat(heights, shape[axis_at] // blocks).reshape([-1 if axis == axis_at else 1 for axis in range(len(shape))])
    return loudness


def gaussian(key, shape, spread, bound, shards=(), dtype=jnp.bfloat16):
    result = spread * jax.random.normal(key, shape, jnp.float32)
    if shards:
        result = result * levels(key, shape, shards, -0.22, 0.18)
    return jnp.clip(result, -bound, bound).astype(dtype)


def setup_inputs(seed: int = 0) -> dict:
    streams_of = jax.random.split(jax.random.key(seed), 8)
    return {
        "tokens": draw_tokens(jax.random.fold_in(streams_of[7], 71), 0),
        "norm_gain": jnp.clip(1.0 + 0.15 * jax.random.normal(streams_of[1], (4, D), jnp.float32), 0.25, 1.75),
        "qkv_weight": gaussian(streams_of[2], (3, D, 3, ATTN_WIDTH), D ** -0.5, 0.1875, ((3, 4),)),
        "qk_gain": jnp.clip(1.0 + 0.15 * jax.random.normal(streams_of[3], (3, 2, HEAD_DIM), jnp.float32), 0.25, 1.75),
        "out_weight": gaussian(streams_of[4], (3, ATTN_WIDTH, D), ATTN_WIDTH ** -0.5, 0.1875, ((1, 4),)),
        "ffn_in": gaussian(streams_of[5], (D, 2, FF), D ** -0.5, 0.1875, ((2, 4),)),
        "ffn_out": gaussian(streams_of[6], (FF, D), FF ** -0.5, 0.125, ((0, 4),)),
    }


def rms_norm(stream, gain_row):
    return stream * lax.rsqrt(lax.optimization_barrier(jnp.mean(stream * stream, axis=-1, keepdims=True)) + 1e-06) * gain_row

def head_norm(vectors, gain_row):
    return vectors * lax.rsqrt(lax.optimization_barrier(jnp.mean(vectors * vectors, axis=-1, keepdims=True)) + 1e-06) * gain_row

def grouped_product(left, right):
    inner = left.shape[-1]
    block = inner // N_TA
    left_blocks = left.reshape(-1, N_TA, block).astype(jnp.float32)
    right_blocks = right.reshape(N_TA, block, -1).astype(jnp.float32)
    parts = jnp.einsum('rgk,gkd->grd', left_blocks, right_blocks)
    rounded = lax.optimization_barrier(parts.astype(jnp.bfloat16))
    return lax.optimization_barrier(jnp.sum(rounded.astype(jnp.float32), axis=0))

def project(normed, weight_block, gain_pair):
    extent = normed.shape
    model_width = extent[-1]
    flat_qkv = jnp.dot(normed.reshape(-1, model_width), weight_block.reshape(model_width, -1), preferred_element_type=jnp.float32)
    head_count = weight_block.shape[-1] // HEAD_DIM
    flat_qkv = flat_qkv.reshape(extent[:4] + (3, head_count, HEAD_DIM))
    queries = head_norm(flat_qkv[..., 0, :, :], gain_pair[0])
    key_rows = head_norm(flat_qkv[..., 1, :, :], gain_pair[1])
    stacked = jnp.stack([queries, key_rows, flat_qkv[..., 2, :, :]], axis=4).astype(jnp.bfloat16)
    return stacked.reshape(extent[:4] + (3, head_count * HEAD_DIM))

def attend(packed, line_axis, causal):
    extent = packed.shape
    head_count = extent[-1] // HEAD_DIM
    split_shape = extent[:4] + (head_count, HEAD_DIM)
    queries = packed[..., 0, :].reshape(split_shape).astype(jnp.float32)
    key_rows = packed[..., 1, :].reshape(split_shape).astype(jnp.float32)
    values = packed[..., 2, :].reshape(split_shape).astype(jnp.float32)
    letters = 'cfyx'
    axis_letter = letters[line_axis]
    query_spec = letters.replace(axis_letter, 'q') + 'hd'
    key_spec = letters.replace(axis_letter, 'k') + 'hd'
    score_spec = letters.replace(axis_letter, '') + 'hqk'
    scores = jnp.einsum(query_spec + ',' + key_spec + '->' + score_spec, queries, key_rows) / math.sqrt(HEAD_DIM)
    exponentials = jnp.exp(scores)
    if causal:
        places = jnp.arange(extent[line_axis])
        exponentials = jnp.where(places[:, None] >= places[None, :], exponentials, jnp.zeros_like(exponentials))
    attn_probs = (exponentials / lax.optimization_barrier(jnp.sum(exponentials, axis=-1, keepdims=True))).astype(jnp.bfloat16)
    attended = jnp.einsum(score_spec + ',' + key_spec + '->' + query_spec, attn_probs.astype(jnp.float32), values)
    return attended.reshape(extent[:4] + (extent[-1],)).astype(jnp.bfloat16)

def attention_pass(stream, gain_row, weight_block, gain_pair, out_block, line_axis, causal):
    map_dim = 2 if line_axis == 1 else 1
    normed = rms_norm(stream, gain_row).astype(jnp.bfloat16)
    blocks = jnp.moveaxis(normed, map_dim, 0)

    def one_block(tile_block):
        restored = jnp.expand_dims(tile_block, map_dim)
        packed = project(restored, weight_block, gain_pair)
        attended = attend(packed, line_axis, causal)
        all_width = attended.shape[-1]
        delta_part = grouped_product(attended.reshape(-1, all_width), out_block)
        return jnp.squeeze(delta_part.reshape(restored.shape[:4] + (out_block.shape[1],)), map_dim)
    deltas = lax.map(one_block, blocks)
    return stream + jnp.moveaxis(deltas, 0, map_dim)

def mlp_block(stream, gain_row, ffn_in, ffn_out):
    normed = rms_norm(stream, gain_row).astype(jnp.bfloat16)
    blocks = jnp.moveaxis(normed, 1, 0)
    model_width = ffn_in.shape[0]
    hidden_width = ffn_in.shape[2]

    def one_frame(frame_tokens):
        flat_tokens = frame_tokens.reshape(-1, model_width)
        both_parts = jnp.dot(flat_tokens, ffn_in.reshape(model_width, -1), preferred_element_type=jnp.float32).reshape(-1, 2, hidden_width)
        hidden = (jax.nn.silu(both_parts[:, 0]) * both_parts[:, 1]).astype(jnp.bfloat16)
        return grouped_product(hidden, ffn_out).reshape(frame_tokens.shape)
    deltas = lax.map(one_frame, blocks)
    return stream + jnp.moveaxis(deltas, 0, 1)

def reference(tokens, norm_gain, qkv_weight, qk_gain, out_weight, ffn_in, ffn_out):
    stream = tokens.astype(jnp.float32)
    for pass_index, line_axis in ((0, 3), (1, 2), (2, 1)):
        stream = attention_pass(stream, norm_gain[pass_index], qkv_weight[pass_index], qk_gain[pass_index], out_weight[pass_index], line_axis, line_axis == 1)
    stream = mlp_block(stream, norm_gain[3], ffn_in, ffn_out)
    return stream.astype(jnp.bfloat16)
```

```python
import functools

import jax
import jax.numpy as jnp
from jax import lax
from jax.experimental import pallas as pl
from jax.experimental.pallas import tpu as pltpu
from jax.sharding import PartitionSpec as P

MESH = pl.DeviceIdType.MESH
BF16, F32 = jnp.bfloat16, jnp.float32
ROWS = 256
UNIT = 128
D = 1024


def place(x, y, z, k):
    return {"ta": x, "ha": (z // 2) * 2 + k, "wa": (z % 2) * 4 + y}


def rows(start, size):
    return pl.ds(pl.multiple_of(start, size), size)


def dot_t(a, b):
    return lax.dot_general(a, b, (((1,), (1,)), ((), ())), preferred_element_type=F32)


def dot(a, b):
    return jnp.dot(a, b, preferred_element_type=F32)


def rms(stream, gain_row):
    return stream * lax.rsqrt(jnp.mean(stream * stream, axis=-1, keepdims=True) + 1e-6) * gain_row


def iotas(shape):
    return lax.broadcasted_iota(jnp.int32, shape, 0), lax.broadcasted_iota(jnp.int32, shape, 1)


def one_hot(source_of):
    out, into = iotas((ROWS, ROWS))
    return jnp.where(source_of(out) == into, 1.0, 0.0).astype(BF16)


def kernel(
    tok,
    attn_src,
    mlp_src,
    norm_gain,
    qk_gain,
    out_ref,
    w_attn,
    w_mlp,
    arrived,
    leaving,
    stream,
    normed,
    partial,
    partial_in,
    qkv,
    heads,
    mask,
    w_send,
    w_recv,
    own_sem,
    t_send,
    t_recv,
    p_send,
    p_recv,
):
    x = lax.axis_index("ta")
    h = lax.axis_index("ha")
    w = lax.axis_index("wa")
    z_hi, k, z_lo, y = h // 2, h % 2, w // 4, w % 4
    z = z_hi * 2 + z_lo
    par = z_lo
    partner = place(x, y, z, 1 - k)

    def w_ref(p, q, start, size):
        if p < 3:
            return w_attn.at[p, :, rows(start, UNIT) if size == UNIT else pl.ds(start, size), rows(q * 128, 128)]
        return w_mlp.at[:, rows(start, UNIT) if size == UNIT else pl.ds(start, size), rows(q * 256, 256)]

    def src_ref(p, start, size):
        return attn_src.at[p, :, pl.ds(start, size), :] if p < 3 else mlp_src.at[:, pl.ds(start, size), :]

    def w_copy(p, d, kind, src, dst, device, send_index):
        return pltpu.make_async_remote_copy(
            src_ref=src,
            dst_ref=dst,
            send_sem=w_send.at[p, send_index],
            recv_sem=w_recv.at[p, d, kind],
            device_id=device,
            device_id_type=MESH,
        )

    def unit_start(kind_start):
        return pl.multiple_of(kind_start, UNIT)

    gamma = pl.multiple_of(512 + par * 256, 256)
    other = pl.multiple_of(512 + (1 - par) * 256, 256)

    def x_copies(p):
        out = []
        for e in (1, 3, 2):
            peer = place((x + e) % 4, y, z, k)
            for kind, start, size in ((0, unit_start(y * UNIT), UNIT), (1, gamma, 256)):
                out.append(
                    w_copy(p, 4 - e, kind, src_ref(p, start, size), w_ref(p, x, start, size), peer, (e - 1) * 2 + kind)
                )
        return out

    def y_copies(p, d):
        q = (x + d) % 4
        block = w_ref(p, q, unit_start(y * UNIT), UNIT)
        return [
            w_copy(p, d, 1 + (4 - e), block, block, place(x, (y + e) % 4, z, k), 6 + (d - 1) * 5 + e - 1)
            for e in (1, 3, 2)
        ]

    def z_copies(p, d):
        q = (x + d) % 4
        first = w_ref(p, q, unit_start(gamma), UNIT)
        second = w_ref(p, q, unit_start(gamma + UNIT), UNIT)
        up, down = place(x, y, (z + 1) % 8, k), place(x, y, (z + 7) % 8, k)
        return [
            w_copy(p, d, 5, first, first, up, 6 + (d - 1) * 5 + 3),
            w_copy(p, d, 6, second, second, down, 6 + (d - 1) * 5 + 4),
        ]

    def w_wait(p, d, kind, start, size):
        block = w_ref(p, (x + d) % 4, start, size)
        w_copy(p, d, kind, block, block, partner, 0).wait_recv()

    def own_copy(p):
        dst = w_attn.at[p, :, :, rows(x * 128, 128)] if p < 3 else w_mlp.at[:, :, rows(x * 256, 256)]
        return pltpu.make_async_copy(attn_src.at[p] if p < 3 else mlp_src, dst, own_sem.at[p])

    def forward(p):
        for d in (1, 3, 2):
            w_wait(p, d, 0, unit_start(y * UNIT), UNIT)
            for copy in y_copies(p, d):
                copy.start()
            w_wait(p, d, 1, gamma, 256)
            for copy in z_copies(p, d):
                copy.start()

    def weights_in(p):
        own_copy(p).wait()
        for d in (1, 3, 2):
            for slot in (1, 2, 3):
                w_wait(p, d, 1 + slot, unit_start(((y + slot) % 4) * UNIT), UNIT)
            w_wait(p, d, 5, unit_start(other), UNIT)
            w_wait(p, d, 6, unit_start(other + UNIT), UNIT)

    def t_copy(stage, index, src, dst, device):
        return pltpu.make_async_remote_copy(
            src_ref=src,
            dst_ref=dst,
            send_sem=t_send.at[stage, index],
            recv_sem=t_recv.at[stage, index],
            device_id=device,
            device_id_type=MESH,
        )

    def copies0():
        out = []
        for d in range(1, 8):
            to = (w + d) % 8
            start = (to % 4) * 64 + (to // 4) * 32
            out.append(
                t_copy(0, d, tok.at[rows(start, 32), :], arrived.at[0, rows(w * 32, 32), :], {"ta": x, "ha": h, "wa": to})
            )
        return out

    def waits0():
        for d in range(1, 8):
            block = arrived.at[0, rows(((w + 8 - d) % 8) * 32, 32), :]
            t_copy(0, d, block, block, partner).wait_recv()

    own_rows = pltpu.make_async_copy(
        tok.at[rows(y * 64 + z_lo * 32, 32), :], arrived.at[0, rows(w * 32, 32), :], own_sem.at[4]
    )

    j = z * 2 + k
    group = z_hi * 4 + k * 2 + z_lo

    def copies1():
        out = []
        for d in range(1, 16):
            to = (j + d) % 16
            to_z, to_k = to // 2, to % 2
            block = (to_z % 2) * 8 + (to_z // 2) * 2 + to_k
            out.append(
                t_copy(
                    1, d, leaving.at[0, rows(block * 16, 16), :], arrived.at[1, rows(group * 16, 16), :], place(x, y, to_z, to_k)
                )
            )
        return out

    def waits1():
        for d in range(1, 16):
            at = (j + 16 - d) % 16
            at_z, at_k = at // 2, at % 2
            slot = (at_z // 2) * 4 + at_k * 2 + at_z % 2
            block = arrived.at[1, rows(slot * 16, 16), :]
            t_copy(1, d, block, block, partner).wait_recv()

    f = x * 4 + y

    def copies2():
        out = []
        for d in range(1, 16):
            to = (f + d) % 16
            to_x, to_y = to // 4, to % 4
            block = to_y * 4 + to_x
            out.append(
                t_copy(2, d, leaving.at[1, rows(block * 16, 16), :], arrived.at[2, rows(f * 16, 16), :], place(to_x, to_y, z, k))
            )
        return out

    def waits2():
        for d in range(1, 16):
            block = arrived.at[2, rows(((f + 16 - d) % 16) * 16, 16), :]
            t_copy(2, d, block, block, partner).wait_recv()

    slot3 = (x % 2) * 8 + z_hi * 2 + k
    at_home = jnp.logical_and(z_hi == y, k == x // 2)

    def copies3():
        out = []
        for dx in range(4):
            for dy in range(4):
                to_x, to_y = (x + dx) % 4, (y + dy) % 4
                copy = pltpu.make_async_remote_copy(
                    src_ref=leaving.at[2, rows((to_x * 4 + to_y) * 16, 16), :],
                    dst_ref=arrived.at[3, rows(slot3 * 16, 16), :],
                    send_sem=t_send.at[3, dx * 4 + dy],
                    recv_sem=t_recv.at[3, slot3],
                    device_id=place(to_x, to_y, y * 2 + z_lo, x // 2),
                    device_id_type=MESH,
                )
                out.append((dx == 0 and dy == 0, copy))
        return out

    def waits3():
        for slot in range(16):

            @pl.when(jnp.logical_not(jnp.logical_and(at_home, slot3 == slot)))
            def _():
                block = arrived.at[3, slot * 16 : slot * 16 + 16, :]
                t_copy(3, slot, block, block, partner).wait_recv()

    def pair_copy(p, index, src, dst):
        return pltpu.make_async_remote_copy(
            src_ref=src,
            dst_ref=dst,
            send_sem=p_send.at[p, index],
            recv_sem=p_recv.at[p, index],
            device_id=partner,
            device_id_type=MESH,
        )

    def share_copy(p):
        return pair_copy(p, 0, normed.at[p, 0], normed.at[p, 1])

    def return_copy(p):
        return pair_copy(p, 1, partial.at[p], partial_in.at[p])

    lane = lax.broadcasted_iota(jnp.int32, (1, 128), 1)
    left = lane < 64

    def head_sums():
        a, b = iotas((256, 256))
        return jnp.where(a // 64 == b // 64, 1.0 / 64.0, 0.0).astype(BF16)

    def project(p, s):
        tokens = normed[p, s]
        for t in range(3):
            for half in range(2):
                cols = slice(half * 256, half * 256 + 256)
                value = dot(tokens, w_attn[p, t, :, cols])
                if t < 2:
                    mean = dot((value * value).astype(BF16), head_sums())
                    value = value * lax.rsqrt(mean + 1e-6) * qk_gain[p, t : t + 1, :]
                qkv[s, t, :, cols] = value.astype(BF16)

    def attend(p, s):
        def pair(i, carry):
            cols = rows(i * 128, 128)
            queries, key_rows = qkv[s, 0, :, cols], qkv[s, 1, :, cols]
            values = jnp.concatenate([qkv[s, 2, :, cols], jnp.ones((ROWS, 128), BF16)], axis=1)
            results = []
            for side in range(2):
                mine = jnp.where(left if side == 0 else jnp.logical_not(left), queries, jnp.zeros_like(queries))
                weights = jnp.exp(dot_t(mine, key_rows)).astype(BF16) * mask[...]
                summed = dot(weights, values)
                results.append(summed[:, :128] / summed[:, 128:])
            heads[s, :, cols] = jnp.where(left, results[0], results[1]).astype(BF16)
            return carry

        lax.fori_loop(0, 4, pair, 0)
        return dot_t(heads[s], w_attn[p, 3])

    def attention(p):
        share_copy(p).start()
        weights_in(p)
        project(p, 0)
        share_copy(p).wait_recv()
        project(p, 1)
        partial[p] = attend(p, 1).astype(BF16)
        return_copy(p).start()
        stream[...] = stream[...] + attend(p, 0)
        return_copy(p).wait_recv()
        stream[...] = stream[...] + partial_in[p].astype(F32)

    def mlp(s):
        tokens = normed[3, s]
        for part in range(4):
            cols = slice(part * 256, part * 256 + 256)
            gate = dot(tokens, w_mlp[0, :, cols])
            up = dot(tokens, w_mlp[1, :, cols])
            qkv[part // 2, part % 2, :, 0:256] = (gate / (1.0 + jnp.exp(-gate)) * up).astype(BF16)
        hidden = jnp.concatenate([qkv[part // 2, part % 2, :, 0:256] for part in range(4)], axis=1)
        return dot_t(hidden, w_mlp[2])

    for copy in copies0():
        copy.start()
    own_rows.start()
    for copy in x_copies(0):
        copy.start()
    for p in range(4):
        own_copy(p).start()
    for copy in x_copies(1):
        copy.start()

    a, b = iotas((ROWS, ROWS))
    mask[...] = jnp.where((a // 8) % 4 == (b // 8) % 4, 1.0, 0.0).astype(BF16)
    own_rows.wait()
    waits0()
    stream[...] = arrived[0].astype(F32)
    normed[0, 0] = rms(stream[...], norm_gain[0:1, :]).astype(BF16)
    forward(0)
    for copy in x_copies(2):
        copy.start()
    attention(0)

    order = one_hot(lambda o: ((o // 128) * 4 + o % 4) * 32 + ((o // 4) % 4) * 8 + (o // 16) % 8)
    leaving[0] = dot(order, stream[...].astype(BF16)).astype(BF16)
    for copy in copies1():
        copy.start()
    own_block = z_lo * 8 + z_hi * 2 + k
    arrived[1, rows(group * 16, 16), :] = leaving[0, rows(own_block * 16, 16), :]
    a, b = iotas((ROWS, ROWS))
    mask[...] = jnp.where(a % 4 == b % 4, 1.0, 0.0).astype(BF16)
    forward(1)
    for copy in x_copies(3):
        copy.start()
    waits1()
    stream[...] = arrived[1].astype(F32)
    normed[1, 0] = rms(stream[...], norm_gain[1:2, :]).astype(BF16)
    attention(1)

    leaving[1] = stream[...].astype(BF16)
    for copy in copies2():
        copy.start()
    arrived[2, rows(f * 16, 16), :] = leaving[1, rows((y * 4 + x) * 16, 16), :]
    a, b = iotas((ROWS, ROWS))
    mask[...] = jnp.where(jnp.logical_and(a % 16 == b % 16, b // 16 <= a // 16), 1.0, 0.0).astype(BF16)
    forward(2)
    waits2()
    stream[...] = arrived[2].astype(F32)
    normed[2, 0] = rms(stream[...], norm_gain[2:3, :]).astype(BF16)
    forward(3)
    attention(2)

    normed[3, 0] = rms(stream[...], norm_gain[3:4, :]).astype(BF16)
    share_copy(3).start()
    weights_in(3)
    share_copy(3).wait_recv()
    partial[3] = mlp(1).astype(BF16)
    return_copy(3).start()
    stream[...] = stream[...] + mlp(0)
    return_copy(3).wait_recv()
    stream[...] = stream[...] + partial_in[3].astype(F32)

    order = one_hot(lambda o: ((o // 64) * 4 + (o // 4) % 4) * 16 + (o % 4) * 4 + (o // 16) % 4)
    leaving[2] = dot(order, stream[...].astype(BF16)).astype(BF16)
    for maybe_self, copy in copies3():
        if maybe_self:

            @pl.when(jnp.logical_not(at_home))
            def _():
                copy.start()

            @pl.when(at_home)
            def _():
                arrived[3, rows(slot3 * 16, 16), :] = leaving[2, rows(f * 16, 16), :]

        else:
            copy.start()
    waits3()
    order = one_hot(lambda o: (((o // 32) % 2) * 8 + o % 8) * 16 + (o // 64) * 4 + (o // 8) % 4)
    out_ref[...] = dot(order, arrived[3]).astype(BF16)

    for copy in copies0() + copies1() + copies2():
        copy.wait_send()
    for maybe_self, copy in copies3():
        if maybe_self:

            @pl.when(jnp.logical_not(at_home))
            def _():
                copy.wait_send()

        else:
            copy.wait_send()
    for p in range(4):
        for copy in x_copies(p):
            copy.wait_send()
        for d in (1, 3, 2):
            for copy in y_copies(p, d) + z_copies(p, d):
                copy.wait_send()
        share_copy(p).wait_send()
        return_copy(p).wait_send()


def local(tokens, norm_gain, qkv_weight, qk_gain, out_weight, ffn_in, ffn_out):
    k = lax.axis_index("ha") % 2
    qkv_half = lax.dynamic_slice_in_dim(qkv_weight, k * 128, 128, 3).transpose(0, 2, 1, 3)
    out_half = lax.dynamic_slice_in_dim(out_weight, k * 128, 128, 1).transpose(0, 2, 1)
    attn_src = jnp.concatenate([qkv_half, out_half[:, None]], axis=1)
    in_half = lax.dynamic_slice_in_dim(ffn_in, k * 256, 256, 2).transpose(1, 0, 2)
    down_half = lax.dynamic_slice_in_dim(ffn_out, k * 256, 256, 0).T
    mlp_src = jnp.concatenate([in_half, down_half[None]], axis=0)
    gains = jnp.tile(qk_gain * jnp.array([0.125, 1.0], F32)[None, :, None], (1, 1, 4))
    vmem, hbm = pl.BlockSpec(memory_space=pltpu.VMEM), pl.BlockSpec(memory_space=pl.ANY)
    result = pl.pallas_call(
        kernel,
        out_shape=jax.ShapeDtypeStruct((ROWS, D), BF16),
        in_specs=[hbm, hbm, hbm, vmem, vmem],
        out_specs=vmem,
        scratch_shapes=[
            pltpu.VMEM((3, 4, D, 512), BF16),
            pltpu.VMEM((3, D, D), BF16),
            pltpu.VMEM((4, ROWS, D), BF16),
            pltpu.VMEM((3, ROWS, D), BF16),
            pltpu.VMEM((ROWS, D), F32),
            pltpu.VMEM((4, 2, ROWS, D), BF16),
            pltpu.VMEM((4, ROWS, D), BF16),
            pltpu.VMEM((4, ROWS, D), BF16),
            pltpu.VMEM((2, 3, ROWS, 512), BF16),
            pltpu.VMEM((2, ROWS, 512), BF16),
            pltpu.VMEM((ROWS, ROWS), BF16),
            pltpu.SemaphoreType.DMA((4, 21)),
            pltpu.SemaphoreType.DMA((4, 4, 7)),
            pltpu.SemaphoreType.DMA((5,)),
            pltpu.SemaphoreType.DMA((4, 16)),
            pltpu.SemaphoreType.DMA((4, 16)),
            pltpu.SemaphoreType.DMA((4, 2)),
            pltpu.SemaphoreType.DMA((4, 2)),
        ],
        compiler_params=pltpu.CompilerParams(has_side_effects=True, vmem_limit_bytes=60 * 2**20),
    )(tokens.reshape(ROWS, D), attn_src, mlp_src, norm_gain, gains)
    return result.reshape(tokens.shape)


def solution(mesh):
    return jax.shard_map(
        local,
        mesh=mesh,
        in_specs=(
            P(None, "ta", "ha", "wa", None),
            P(),
            P(None, None, None, "ta"),
            P(),
            P(None, "ta", None),
            P(None, None, "ta"),
            P("ta", None),
        ),
        out_specs=P(None, "ta", "ha", "wa", None),
        check_vma=False,
    )
```

```python
import functools

import jax
import jax.numpy as jnp
from jax import lax
from jax.experimental import pallas as pl
from jax.experimental.pallas import tpu as pltpu
from jax.sharding import PartitionSpec as P

MESH = pl.DeviceIdType.MESH
BF16, F32 = jnp.bfloat16, jnp.float32
ROWS = 256
UNIT = 128
D = 1024


def place(x, y, z, k):
    return {"ta": x, "ha": (z // 2) * 2 + k, "wa": (z % 2) * 4 + y}


def rows(start, size):
    return pl.ds(pl.multiple_of(start, size), size)


def dot_t(a, b):
    return lax.dot_general(a, b, (((1,), (1,)), ((), ())), preferred_element_type=F32)


def dot(a, b):
    return jnp.dot(a, b, preferred_element_type=F32)


def rms(stream, gain_row):
    return stream * lax.rsqrt(jnp.mean(stream * stream, axis=-1, keepdims=True) + 1e-6) * gain_row


def iotas(shape):
    return lax.broadcasted_iota(jnp.int32, shape, 0), lax.broadcasted_iota(jnp.int32, shape, 1)


def one_hot(source_of):
    out, into = iotas((ROWS, ROWS))
    return jnp.where(source_of(out) == into, 1.0, 0.0).astype(BF16)


def kernel(
    tok,
    qkv_src,
    out_src,
    in_src,
    down_src,
    norm_gain,
    qk_gain,
    out_ref,
    w_attn,
    w_out,
    w_in,
    w_down,
    arrived,
    leaving,
    stream,
    normed,
    partial,
    partial_in,
    qkv,
    heads,
    hidden,
    mask,
    w_send,
    w_recv,
    own_sem,
    t_send,
    t_recv,
    p_send,
    p_recv,
    hello,
):
    x = lax.axis_index("ta")
    h = lax.axis_index("ha")
    w = lax.axis_index("wa")
    z_hi, k, z_lo, y = h // 2, h % 2, w // 4, w % 4
    z = z_hi * 2 + z_lo
    phase = z_hi + 2 * z_lo + k
    partner = place(x, y, z, 1 - k)

    def both(p, d, start, size):
        if p < 3:
            return w_attn.at[p, d, :, pl.ds(start, size), :], w_out.at[p, d * 128 : d * 128 + 128, pl.ds(start, size)]
        return w_in.at[d, :, pl.ds(start, size), :], w_down.at[d * 256 : d * 256 + 256, pl.ds(start, size)]

    def both_src(p, start, size):
        if p < 3:
            return (
                qkv_src.at[p, :, pl.ds(start, size), rows(k * 128, 128)],
                out_src.at[p, rows(k * 128, 128), pl.ds(start, size)],
            )
        return (
            in_src.at[:, pl.ds(start, size), rows(k * 256, 256)],
            down_src.at[rows(k * 256, 256), pl.ds(start, size)],
        )

    def w_copies(p, d, kind, src, dst, device):
        return [
            pltpu.make_async_remote_copy(
                src_ref=a,
                dst_ref=b,
                send_sem=w_send.at[p],
                recv_sem=w_recv.at[p, d, kind],
                device_id=device,
                device_id_type=MESH,
            )
            for a, b in zip(src, dst)
        ]

    def w_total(p, d, kind, units):
        block = w_down.at[0 : (64 if p < 3 else 96) * units, :]
        return w_copies(p, d, kind, [block], [block], partner)[0]

    def w_wait(p, d, kind, units):
        w_total(p, d, kind, units).wait_recv()

    def unit(start):
        return pl.multiple_of(start, UNIT)

    gamma = pl.multiple_of(512 + z_lo * 256, 256)

    def x_send(p, kind, steps=(1, 3, 2)):
        for e in steps:
            peer = place((x + e) % 4, y, z, k)
            start, size = ((unit(y * UNIT), UNIT), (gamma, 256))[kind]
            for copy in w_copies(p, 4 - e, kind, both_src(p, start, size), both(p, 4 - e, start, size), peer):
                copy.start()

    def forward_y(p, *quarters):
        for d in quarters:
            w_wait(p, d, 0, 1)
            block = both(p, d, unit(y * UNIT), UNIT)
            for e in (1, 3, 2):
                for copy in w_copies(p, d, 2, block, block, place(x, (y + e) % 4, z, k)):
                    copy.start()

    def forward_z(p, *quarters):
        for d in quarters:
            w_wait(p, d, 1, 2)
            for side, step in ((0, 1), (1, 7)):
                block = both(p, d, unit(gamma + side * UNIT), UNIT)
                for copy in w_copies(p, d, 2, block, block, place(x, y, (z + step) % 8, k)):
                    copy.start()

    def own_copies(p):
        return [
            pltpu.make_async_copy(a, b, own_sem.at[p, i]) for i, (a, b) in enumerate(zip(both_src(p, 0, D), both(p, 0, 0, D)))
        ]

    def weights_in(p, d):
        @pl.when(d == 0)
        def _():
            for copy in own_copies(p):
                copy.wait()

        @pl.when(d > 0)
        def _():
            w_wait(p, d, 2, 5)

    def t_copy(stage, src, dst, device):
        return pltpu.make_async_remote_copy(
            src_ref=src,
            dst_ref=dst,
            send_sem=t_send.at[stage],
            recv_sem=t_recv.at[stage],
            device_id=device,
            device_id_type=MESH,
        )

    def copies0():
        out = []
        for d in range(1, 8):
            to = (w + d) % 8
            start = (to % 4) * 64 + (to // 4) * 32
            out.append(
                t_copy(0, tok.at[rows(start, 32), :], arrived.at[0, rows(w * 32, 32), :], {"ta": x, "ha": h, "wa": to})
            )
        return out

    def t_total(stage, count):
        block = arrived.at[stage, 0:count, :]
        return t_copy(stage, block, block, partner)

    own_rows = pltpu.make_async_copy(
        tok.at[rows(y * 64 + z_lo * 32, 32), :], arrived.at[0, rows(w * 32, 32), :], own_sem.at[4, 0]
    )

    j = z * 2 + k
    group = z_hi * 4 + k * 2 + z_lo

    def copies1():
        out = []
        for d in range(1, 16):
            to = (j + d) % 16
            to_z, to_k = to // 2, to % 2
            block = (to_z % 2) * 8 + (to_z // 2) * 2 + to_k
            out.append(
                t_copy(
                    1, leaving.at[0, rows(block * 16, 16), :], arrived.at[1, rows(group * 16, 16), :], place(x, y, to_z, to_k)
                )
            )
        return out

    f = x * 4 + y

    def copies2():
        out = []
        for d in range(1, 16):
            to = (f + d) % 16
            to_x, to_y = to // 4, to % 4
            block = ((to_y + phase) % 4) * 4 + to_x
            out.append(
                t_copy(2, leaving.at[1, rows(block * 16, 16), :], arrived.at[2, rows(f * 16, 16), :], place(to_x, to_y, z, k))
            )
        return out

    slot3 = (x % 2) * 8 + z_hi * 2 + k
    to_hi = (y + phase) % 4
    at_home = jnp.logical_and(z_hi == to_hi, k == x // 2)

    def copies3():
        out = []
        for dx in range(4):
            for dy in range(4):
                to_x, to_y = (x + dx) % 4, (y + dy) % 4
                copy = t_copy(
                    3,
                    leaving.at[2, rows((to_x * 4 + to_y) * 16, 16), :],
                    arrived.at[3, rows(slot3 * 16, 16), :],
                    place(to_x, to_y, to_hi * 2 + z_lo, x // 2),
                )
                out.append((dx == 0 and dy == 0, copy))
        return out

    def all_home(act):
        @pl.when(at_home)
        def _():
            act(t_total(3, 240))

        @pl.when(jnp.logical_not(at_home))
        def _():
            act(t_total(3, 256))

    def pair_copy(p, index, src, dst):
        return pltpu.make_async_remote_copy(
            src_ref=src,
            dst_ref=dst,
            send_sem=p_send.at[p, index],
            recv_sem=p_recv.at[p, index],
            device_id=partner,
            device_id_type=MESH,
        )

    def share_copy(p):
        return pair_copy(p, 0, normed.at[p, 0:ROWS, :], normed.at[p, ROWS : 2 * ROWS, :])

    def return_copy(p):
        return pair_copy(p, 1, partial.at[p], partial_in.at[p])

    def greet(stage, peers):
        for peer in peers:
            pl.semaphore_signal(hello.at[stage], inc=1, device_id=peer, device_id_type=MESH)

    lane = lax.broadcasted_iota(jnp.int32, (1, 128), 1)
    left = lane < 64

    def project(p, d):
        tokens = normed[p]
        both_heads = dot(tokens, jnp.concatenate([w_attn[p, d, 0], w_attn[p, d, 1]], axis=1))
        a, b = iotas((256, 256))
        gain = jnp.concatenate([qk_gain[p, 0:1, :] * 0.125] * 2 + [qk_gain[p, 1:2, :]] * 2, axis=1)
        sums = jnp.where(a // 64 == b // 64, 1.0 / 64.0, 0.0).astype(BF16)
        mean = dot((both_heads * both_heads).astype(BF16), sums)
        qkv[:, 0:256] = (both_heads * lax.rsqrt(mean + 1e-6) * gain).astype(BF16)
        qkv[:, 256:384] = dot(tokens, w_attn[p, d, 2]).astype(BF16)

    def attend(d):
        for s in range(2):
            r = slice(s * ROWS, s * ROWS + ROWS)
            queries, key_rows = qkv[r, 0:128], qkv[r, 128:256]
            values = jnp.concatenate([qkv[r, 256:384], jnp.ones((ROWS, 128), BF16)], axis=1)
            results = []
            for side in range(2):
                mine = jnp.where(left if side == 0 else jnp.logical_not(left), queries, jnp.zeros_like(queries))
                weights = jnp.exp(dot_t(mine, key_rows)).astype(BF16) * mask[...]
                summed = dot(weights, values)
                results.append(summed[:, :128] / summed[:, 128:])
            heads[r, rows(d * 128, 128)] = jnp.where(left, results[0], results[1]).astype(BF16)

    def quarters(relays, work):
        def step(i, carry):
            work(i + i // 2 - 2 * (i // 3))
            for at, relay in relays:
                pl.when(i == at)(relay)
            return carry

        lax.fori_loop(0, 4, step, 0)

    def attention(p, *relays):
        def work(d):
            weights_in(p, d)
            project(p, d)
            attend(d)

        quarters(relays, work)
        finish(p, heads, w_out[p])

    def mlp_quarter(d):
        weights_in(3, d)
        tokens = normed[3]
        gate = dot(tokens, w_in[d, 0])
        up = dot(tokens, w_in[d, 1])
        hidden[:, rows(d * 256, 256)] = (gate / (1.0 + jnp.exp(-gate)) * up).astype(BF16)

    def finish(p, left_ref, right_ref):
        partial[p] = dot(left_ref[ROWS:, :], right_ref).astype(BF16)
        return_copy(p).start()
        stream[...] = stream[...] + dot(left_ref[:ROWS, :], right_ref)
        return_copy(p).wait_recv()
        stream[...] = stream[...] + partial_in[p].astype(F32)

    def begin(p):
        normed[p, 0:ROWS, :] = rms(stream[...], norm_gain[p : p + 1, :]).astype(BF16)
        share_copy(p).start()

    for p in range(4):
        for copy in own_copies(p):
            copy.start()
    own_rows.start()
    barrier = pltpu.get_barrier_semaphore()
    greeted = [place((x + e) % 4, y, z, k) for e in (1, 2, 3)]
    greeted += [{"ta": x, "ha": h, "wa": (w + d) % 8} for d in range(1, 8)]
    greeted += [partner, place(x, y, (z + 7 + 2 * z_lo) % 8, k)]
    for peer in greeted:
        pl.semaphore_signal(barrier, inc=1, device_id=peer, device_id_type=MESH)
    pl.semaphore_wait(barrier, len(greeted))
    for copy in copies0():
        copy.start()
    for p in range(2):
        for kind in range(2):
            x_send(p, kind)
    greet(0, [place(x, y, (z + 1) % 8, k), place(x, y, (z + 7) % 8, k)])

    a, b = iotas((ROWS, ROWS))
    mask[...] = jnp.where((a // 8) % 4 == (b // 8) % 4, 1.0, 0.0).astype(BF16)
    pl.semaphore_wait(hello.at[0], 2)
    greet(1, [place(x, y, (z + 2) % 8, k), place(x, y, (z + 6) % 8, k)])
    forward_y(0, 1, 3)
    own_rows.wait()
    t_total(0, 224).wait_recv()
    stream[...] = arrived[0].astype(F32)
    begin(0)
    forward_y(0, 2)
    pl.semaphore_wait(hello.at[1], 2)
    greet(2, [partner])
    share_copy(0).wait_recv()

    def late():
        x_send(2, 0)
        x_send(2, 1)
        forward_y(1, 1, 3)

    attention(0, (0, lambda: forward_z(0, 1, 3)), (1, lambda: forward_z(0, 2)), (2, late))
    pl.semaphore_wait(hello.at[2], 1)

    order = one_hot(lambda o: ((o // 128) * 4 + o % 4) * 32 + ((o // 4) % 4) * 8 + (o // 16) % 8)
    leaving[0] = dot(order, stream[...].astype(BF16)).astype(BF16)
    for copy in copies1():
        copy.start()
    x_send(3, 0)
    own_block = z_lo * 8 + z_hi * 2 + k
    arrived[1, rows(group * 16, 16), :] = leaving[0, rows(own_block * 16, 16), :]
    a, b = iotas((ROWS, ROWS))
    mask[...] = jnp.where(a % 4 == b % 4, 1.0, 0.0).astype(BF16)
    forward_y(1, 2)
    forward_z(1, 1, 3, 2)
    t_total(1, 240).wait_recv()
    stream[...] = arrived[1].astype(F32)
    begin(1)
    forward_y(2, 1, 3)
    share_copy(1).wait_recv()
    attention(1, (0, lambda: forward_y(2, 2)), (2, lambda: forward_z(2, 1, 3)))

    leaving[1] = stream[...].astype(BF16)
    for copy in copies2():
        copy.start()
    x_send(3, 1, (1, 3))
    arrived[2, rows(f * 16, 16), :] = leaving[1, rows((((y + phase) % 4) * 4 + x) * 16, 16), :]
    a, b = iotas((ROWS, ROWS))
    mask[...] = jnp.where(jnp.logical_and(a % 16 == b % 16, b // 16 <= a // 16), 1.0, 0.0).astype(BF16)
    forward_z(2, 2)
    forward_y(3, 1, 3, 2)
    t_total(2, 240).wait_recv()
    x_send(3, 1, (2,))
    stream[...] = arrived[2].astype(F32)
    begin(2)
    share_copy(2).wait_recv()
    attention(2, (0, lambda: forward_z(3, 1)), (1, lambda: forward_z(3, 3)))

    begin(3)
    share_copy(3).wait_recv()
    quarters(((1, lambda: forward_z(3, 2)),), mlp_quarter)
    finish(3, hidden, w_down[...])

    order = one_hot(lambda o: ((o // 64) * 4 + (o // 4) % 4) * 16 + (o % 4) * 4 + (o // 16) % 4)
    leaving[2] = dot(order, stream[...].astype(BF16)).astype(BF16)
    for maybe_self, copy in copies3():
        if maybe_self:

            @pl.when(jnp.logical_not(at_home))
            def _():
                copy.start()

            @pl.when(at_home)
            def _():
                arrived[3, rows(slot3 * 16, 16), :] = leaving[2, rows(f * 16, 16), :]

        else:
            copy.start()
    all_home(lambda copy: copy.wait_recv())
    order = one_hot(lambda o: (((o // 32) % 2) * 8 + o % 8) * 16 + (o // 64) * 4 + (o // 8) % 4)
    out_ref[...] = dot(order, arrived[3]).astype(BF16)

    t_total(0, 224).wait_send()
    t_total(1, 240).wait_send()
    t_total(2, 240).wait_send()
    all_home(lambda copy: copy.wait_send())
    for p in range(4):
        for _ in range(3):
            w_total(p, 0, 0, 8).wait_send()
        share_copy(p).wait_send()
        return_copy(p).wait_send()


def local(tokens, norm_gain, qkv_weight, qk_gain, out_weight, ffn_in, ffn_out):
    qkv_src = qkv_weight.transpose(0, 2, 1, 3)
    in_src = ffn_in.transpose(1, 0, 2)
    vmem, hbm = pl.BlockSpec(memory_space=pltpu.VMEM), pl.BlockSpec(memory_space=pl.ANY)
    result = pl.pallas_call(
        kernel,
        out_shape=jax.ShapeDtypeStruct((ROWS, D), BF16),
        in_specs=[hbm, hbm, hbm, hbm, hbm, vmem, vmem],
        out_specs=vmem,
        scratch_shapes=[
            pltpu.VMEM((3, 4, 3, D, 128), BF16),
            pltpu.VMEM((3, 512, D), BF16),
            pltpu.VMEM((4, 2, D, 256), BF16),
            pltpu.VMEM((D, D), BF16),
            pltpu.VMEM((4, ROWS, D), BF16),
            pltpu.VMEM((3, ROWS, D), BF16),
            pltpu.VMEM((ROWS, D), F32),
            pltpu.VMEM((4, 2 * ROWS, D), BF16),
            pltpu.VMEM((4, ROWS, D), BF16),
            pltpu.VMEM((4, ROWS, D), BF16),
            pltpu.VMEM((2 * ROWS, 384), BF16),
            pltpu.VMEM((2 * ROWS, 512), BF16),
            pltpu.VMEM((2 * ROWS, D), BF16),
            pltpu.VMEM((ROWS, ROWS), BF16),
            pltpu.SemaphoreType.DMA((4,)),
            pltpu.SemaphoreType.DMA((4, 4, 3)),
            pltpu.SemaphoreType.DMA((5, 2)),
            pltpu.SemaphoreType.DMA((4,)),
            pltpu.SemaphoreType.DMA((4,)),
            pltpu.SemaphoreType.DMA((4, 2)),
            pltpu.SemaphoreType.DMA((4, 2)),
            pltpu.SemaphoreType.REGULAR((3,)),
        ],
        compiler_params=pltpu.CompilerParams(collective_id=0, has_side_effects=True, vmem_limit_bytes=60 * 2**20),
    )(tokens.reshape(ROWS, D), qkv_src, out_weight, in_src, ffn_out, norm_gain, qk_gain)
    return result.reshape(tokens.shape)


def solution(mesh):
    return jax.shard_map(
        local,
        mesh=mesh,
        in_specs=(
            P(None, "ta", "ha", "wa", None),
            P(),
            P(None, None, None, "ta"),
            P(),
            P(None, "ta", None),
            P(None, None, "ta"),
            P("ta", None),
        ),
        out_specs=P(None, "ta", "ha", "wa", None),
        check_vma=False,
    )
```

```python
import functools

import jax
import jax.numpy as jnp
from jax import lax
from jax.experimental import pallas as pl
from jax.experimental.pallas import tpu as pltpu
from jax.sharding import PartitionSpec as P

MESH = pl.DeviceIdType.MESH
BF16, F32 = jnp.bfloat16, jnp.float32
ROWS = 256
UNIT = 128
D = 1024


def place(x, y, z, k):
    return {"ta": x, "ha": (z // 2) * 2 + k, "wa": (z % 2) * 4 + y}


def rows(start, size):
    return pl.ds(pl.multiple_of(start, size), size)


def dot_t(a, b):
    return lax.dot_general(a, b, (((1,), (1,)), ((), ())), preferred_element_type=F32)


def dot(a, b):
    return jnp.dot(a, b, preferred_element_type=F32)


def rms(stream, gain_row):
    return stream * lax.rsqrt(jnp.mean(stream * stream, axis=-1, keepdims=True) + 1e-6) * gain_row


def iotas(shape):
    return lax.broadcasted_iota(jnp.int32, shape, 0), lax.broadcasted_iota(jnp.int32, shape, 1)


def one_hot(source_of):
    out, into = iotas((ROWS, ROWS))
    return jnp.where(source_of(out) == into, 1.0, 0.0).astype(BF16)


def kernel(
    tok,
    qkv_src,
    out_src,
    in_src,
    down_src,
    norm_gain,
    qk_gain,
    out_ref,
    w_attn,
    w_out,
    w_in,
    w_down,
    arrived,
    leaving,
    stream,
    normed,
    partial,
    partial_in,
    qkv,
    heads,
    hidden,
    mask,
    w_send,
    w_recv,
    own_sem,
    t_send,
    t_recv,
    p_send,
    p_recv,
    hello,
):
    x = lax.axis_index("ta")
    h = lax.axis_index("ha")
    w = lax.axis_index("wa")
    z_hi, k, z_lo, y = h // 2, h % 2, w // 4, w % 4
    z = z_hi * 2 + z_lo
    partner = place(x, y, z, 1 - k)

    def both(p, d, start, size):
        if p < 3:
            return w_attn.at[p, d, :, pl.ds(start, size), :], w_out.at[p, d * 128 : d * 128 + 128, pl.ds(start, size)]
        return w_in.at[d, :, pl.ds(start, size), :], w_down.at[d * 256 : d * 256 + 256, pl.ds(start, size)]

    def both_src(p, start, size):
        if p < 3:
            return (
                qkv_src.at[p, :, pl.ds(start, size), rows(k * 128, 128)],
                out_src.at[p, rows(k * 128, 128), pl.ds(start, size)],
            )
        return (
            in_src.at[:, pl.ds(start, size), rows(k * 256, 256)],
            down_src.at[rows(k * 256, 256), pl.ds(start, size)],
        )

    def w_copies(p, d, kind, src, dst, device):
        return [
            pltpu.make_async_remote_copy(
                src_ref=a,
                dst_ref=b,
                send_sem=w_send.at[p],
                recv_sem=w_recv.at[p, d, kind],
                device_id=device,
                device_id_type=MESH,
            )
            for a, b in zip(src, dst)
        ]

    def w_total(p, d, kind, units):
        block = w_down.at[0 : (64 if p < 3 else 96) * units, :]
        return w_copies(p, d, kind, [block], [block], partner)[0]

    def w_wait(p, d, kind, units):
        w_total(p, d, kind, units).wait_recv()

    def unit(start):
        return pl.multiple_of(start, UNIT)

    gamma = pl.multiple_of(512 + z_lo * 256, 256)

    def start_all(copies):
        for copy in copies:
            copy.start()

    def x_send(p, kind):
        for e in (1, 3):
            start, size = ((unit(y * UNIT), UNIT), (gamma, 256))[kind]
            start_all(
                w_copies(p, 4 - e, kind, both_src(p, start, size), both(p, 4 - e, start, size), place((x + e) % 4, y, z, k))
            )

    def x_relay(p, d, kind, start):
        block, there = both(p, d, start, UNIT), both(p, 2, start, UNIT)
        start_all(w_copies(p, 2, kind, block, there, place((x + 4 - d) % 4, y, z, k)))

    def forward_y(p, *quarters):
        for d in quarters:
            w_wait(p, d, 0, 1)
            block = both(p, d, unit(y * UNIT), UNIT)
            if d != 2:
                pl.when(k == (0 if d == 3 else 1))(lambda: x_relay(p, d, 0, unit(y * UNIT)))
            for e in (1, 3, 2):
                start_all(w_copies(p, d, 2, block, block, place(x, (y + e) % 4, z, k)))

    def forward_z(p, *quarters):
        for d in quarters:
            w_wait(p, d, 1, 2)
            if d != 2:
                x_relay(p, d, 1, unit(gamma if d == 3 else gamma + UNIT))
            for side, step in ((0, 1), (1, 7)):
                block = both(p, d, unit(gamma + side * UNIT), UNIT)
                start_all(w_copies(p, d, 2, block, block, place(x, y, (z + step) % 8, k)))

    def own_copies(p):
        return [
            pltpu.make_async_copy(a, b, own_sem.at[p, i]) for i, (a, b) in enumerate(zip(both_src(p, 0, D), both(p, 0, 0, D)))
        ]

    def own_in(p):
        for copy in own_copies(p):
            copy.wait()

    def weights_in(p, d):
        w_wait(p, d, 2, 5)

    def t_copy(stage, src, dst, device):
        return pltpu.make_async_remote_copy(
            src_ref=src,
            dst_ref=dst,
            send_sem=t_send.at[stage],
            recv_sem=t_recv.at[stage],
            device_id=device,
            device_id_type=MESH,
        )

    def copies0():
        out = []
        for d in range(1, 8):
            to = (w + d) % 8
            start = (to % 4) * 64 + (to // 4) * 32
            out.append(
                t_copy(0, tok.at[rows(start, 32), :], arrived.at[0, rows(w * 32, 32), :], {"ta": x, "ha": h, "wa": to})
            )
        return out

    def t_total(stage, count):
        block = arrived.at[stage, 0:count, :]
        return t_copy(stage, block, block, partner)

    own_rows = pltpu.make_async_copy(
        tok.at[rows(y * 64 + z_lo * 32, 32), :], arrived.at[0, rows(w * 32, 32), :], own_sem.at[4, 0]
    )

    j = z * 2 + k
    group = z_hi * 4 + k * 2 + z_lo

    def copies1():
        out = []
        for d in range(1, 16):
            to = (j + d) % 16
            to_z, to_k = to // 2, to % 2
            block = (to_z % 2) * 8 + (to_z // 2) * 2 + to_k
            out.append(
                t_copy(
                    1, leaving.at[0, rows(block * 16, 16), :], arrived.at[1, rows(group * 16, 16), :], place(x, y, to_z, to_k)
                )
            )
        return out

    f = x * 4 + y

    def turn(to_y):
        return (to_y + 2 * z_lo + k) % 4

    def moved(c, to_x):
        half_way = jnp.where(c == 2, jnp.where(to_x // 2 == 0, 1, 3), jnp.where(to_x % 2 == 0, c, 0))
        return jnp.where(c == 0, 0, half_way)

    def copies2():
        out = []
        for d in range(16):
            to = (f + d) % 16
            to_x, to_y = to // 4, to % 4
            c = turn(to_y)
            block = ((z_hi + c) % 4) * 4 + to_x
            to_z = ((z_hi + moved(c, to_x)) % 4) * 2 + z_lo
            copy = t_copy(2, leaving.at[1, rows(block * 16, 16), :], arrived.at[2, rows(f * 16, 16), :], place(to_x, to_y, to_z, k))
            out.append((d == 0, copy))
        return out

    my_turn = turn(y)
    stays = moved(my_turn, x) == 0
    from_hi = (z_hi + 4 - moved(my_turn, x)) % 4

    slot3 = (x % 2) * 8 + from_hi * 2 + k
    to_hi = (from_hi + my_turn) % 4
    at_home = jnp.logical_and(z_hi == to_hi, k == x // 2)

    def copies3():
        out = []
        for dx in range(4):
            for dy in range(4):
                to_x, to_y = (x + dx) % 4, (y + dy) % 4
                copy = t_copy(
                    3,
                    leaving.at[2, rows((to_x * 4 + to_y) * 16, 16), :],
                    arrived.at[3, rows(slot3 * 16, 16), :],
                    place(to_x, to_y, to_hi * 2 + z_lo, x // 2),
                )
                out.append((dx == 0 and dy == 0, copy))
        return out

    def unless(kept, stage, act):
        pl.when(kept)(lambda: act(t_total(stage, 240)))
        pl.when(jnp.logical_not(kept))(lambda: act(t_total(stage, 256)))

    def send_all(copies, kept, keep):
        for maybe_self, copy in copies:
            if maybe_self:
                pl.when(jnp.logical_not(kept))(copy.start)
                pl.when(kept)(keep)
            else:
                copy.start()

    def pair_copy(p, index, src, dst):
        return pltpu.make_async_remote_copy(
            src_ref=src,
            dst_ref=dst,
            send_sem=p_send.at[p, index],
            recv_sem=p_recv.at[p, index],
            device_id=partner,
            device_id_type=MESH,
        )

    def share_copy(p):
        return pair_copy(p, 0, normed.at[p, 0:ROWS, :], normed.at[p, ROWS : 2 * ROWS, :])

    def return_copy(p):
        return pair_copy(p, 1, partial.at[p], partial_in.at[p])

    def greet(stage, peers):
        for peer in peers:
            pl.semaphore_signal(hello.at[stage], inc=1, device_id=peer, device_id_type=MESH)

    lane = lax.broadcasted_iota(jnp.int32, (1, 128), 1)
    left = lane < 64

    own, other, all_rows = slice(0, ROWS), slice(ROWS, 2 * ROWS), slice(0, 2 * ROWS)

    def project(p, d, r):
        tokens = normed[p, r, :]
        both_heads = dot(tokens, jnp.concatenate([w_attn[p, d, 0], w_attn[p, d, 1]], axis=1))
        a, b = iotas((256, 256))
        gain = jnp.concatenate([qk_gain[p, 0:1, :] * 0.125] * 2 + [qk_gain[p, 1:2, :]] * 2, axis=1)
        sums = jnp.where(a // 64 == b // 64, 1.0 / 64.0, 0.0).astype(BF16)
        mean = dot((both_heads * both_heads).astype(BF16), sums)
        qkv[r, 256:384] = dot(tokens, w_attn[p, d, 2]).astype(BF16)
        qkv[r, 0:256] = (both_heads * lax.rsqrt(mean + 1e-6) * gain).astype(BF16)

    def attend(d, r):
        queries, key_rows = qkv[r, 0:128], qkv[r, 128:256]
        values = jnp.concatenate([qkv[r, 256:384], jnp.ones((ROWS, 128), BF16)], axis=1)
        results = []
        for side in range(2):
            mine = jnp.where(left if side == 0 else jnp.logical_not(left), queries, jnp.zeros_like(queries))
            weights = jnp.exp(dot_t(mine, key_rows)).astype(BF16) * mask[...]
            summed = dot(weights, values)
            results.append(summed[:, :128] / summed[:, 128:])
        heads[r, d * 128 : d * 128 + 128] = jnp.where(left, results[0], results[1]).astype(BF16)

    def attention(p, relay0=None, relay1=None, relay3=None):
        own_in(p)
        project(p, 0, own)
        attend(0, own)
        share_copy(p).wait_recv()
        project(p, 0, other)
        attend(0, other)
        for relay, d in ((relay0, 1), (relay1, 3)):
            if relay is not None:
                relay()
            weights_in(p, d)
            project(p, d, all_rows)
            attend(d, own)
            attend(d, other)
        if relay3 is not None:
            relay3()
        weights_in(p, 2)
        project(p, 2, other)
        attend(2, other)
        partial[p] = dot(heads[other, :], w_out[p]).astype(BF16)
        return_copy(p).start()
        project(p, 2, own)
        attend(2, own)
        finish(p, heads, w_out[p])

    def mlp_quarter(d, r):
        tokens = normed[3, r, :]
        gate = dot(tokens, w_in[d, 0])
        up = dot(tokens, w_in[d, 1])
        hidden[r, d * 256 : d * 256 + 256] = (gate / (1.0 + jnp.exp(-gate)) * up).astype(BF16)

    def mlp():
        own_in(3)
        mlp_quarter(0, own)
        share_copy(3).wait_recv()
        mlp_quarter(0, other)
        for d in (1, 3):
            weights_in(3, d)
            mlp_quarter(d, all_rows)
        weights_in(3, 2)
        mlp_quarter(2, other)
        partial[3] = dot(hidden[other, :], w_down[...]).astype(BF16)
        return_copy(3).start()
        mlp_quarter(2, own)
        finish(3, hidden, w_down[...])

    def finish(p, left_ref, right_ref):
        stream[...] = stream[...] + dot(left_ref[own, :], right_ref)
        return_copy(p).wait_recv()
        stream[...] = stream[...] + partial_in[p].astype(F32)

    def begin(p):
        normed[p, 0:ROWS, :] = rms(stream[...], norm_gain[p : p + 1, :]).astype(BF16)
        share_copy(p).start()

    for p in range(4):
        for copy in own_copies(p):
            copy.start()
    own_rows.start()
    barrier = pltpu.get_barrier_semaphore()
    greeted = [place((x + e) % 4, y, z, k) for e in (1, 2, 3)]
    greeted += [{"ta": x, "ha": h, "wa": (w + d) % 8} for d in range(1, 8)]
    greeted += [partner, place(x, y, (z + 7 + 2 * z_lo) % 8, k)]
    for peer in greeted:
        pl.semaphore_signal(barrier, inc=1, device_id=peer, device_id_type=MESH)
    pl.semaphore_wait(barrier, len(greeted))
    start_all(copies0())
    x_send(0, 0)
    x_send(0, 1)
    greet(0, [place(x, y, (z + 1) % 8, k), place(x, y, (z + 7) % 8, k)])

    a, b = iotas((ROWS, ROWS))
    mask[...] = jnp.where((a // 8) % 4 == (b // 8) % 4, 1.0, 0.0).astype(BF16)
    pl.semaphore_wait(hello.at[0], 2)
    greet(1, [place(x, y, (z + 2) % 8, k), place(x, y, (z + 6) % 8, k)])
    forward_y(0, 1, 3)
    x_send(1, 0)
    own_rows.wait()
    t_total(0, 224).wait_recv()
    stream[...] = arrived[0].astype(F32)
    begin(0)
    pl.semaphore_wait(hello.at[1], 2)
    greet(2, [partner])

    def relays00():
        forward_z(0, 1, 3)
        x_send(1, 1)
        forward_y(0, 2)

    def relays01():
        forward_z(0, 2)
        forward_y(1, 1, 3)
        x_send(2, 0)

    def relays02():
        forward_z(1, 1, 3)
        x_send(2, 1)
        forward_y(1, 2)

    attention(0, relays00, relays01, relays02)
    pl.semaphore_wait(hello.at[2], 1)

    order = one_hot(lambda o: ((o // 128) * 4 + o % 4) * 32 + ((o // 4) % 4) * 8 + (o // 16) % 8)
    leaving[0] = dot(order, stream[...].astype(BF16)).astype(BF16)
    start_all(copies1())
    own_block = z_lo * 8 + z_hi * 2 + k
    arrived[1, rows(group * 16, 16), :] = leaving[0, rows(own_block * 16, 16), :]
    a, b = iotas((ROWS, ROWS))
    mask[...] = jnp.where(a % 4 == b % 4, 1.0, 0.0).astype(BF16)
    forward_z(1, 2)
    forward_y(2, 1, 3)
    x_send(3, 0)
    t_total(1, 240).wait_recv()
    stream[...] = arrived[1].astype(F32)
    begin(1)
    forward_z(2, 1, 3)
    x_send(3, 1)
    forward_y(2, 2)

    attention(1, None, lambda: forward_z(2, 2), lambda: forward_y(3, 1))

    leaving[1] = stream[...].astype(BF16)

    def keep2():
        arrived[2, rows(f * 16, 16), :] = leaving[1, rows((((z_hi + my_turn) % 4) * 4 + x) * 16, 16), :]

    send_all(copies2(), stays, keep2)
    a, b = iotas((ROWS, ROWS))
    mask[...] = jnp.where(jnp.logical_and(a % 16 == b % 16, b // 16 <= a // 16), 1.0, 0.0).astype(BF16)
    unless(stays, 2, lambda copy: copy.wait_recv())
    forward_z(3, 1, 3)
    forward_y(3, 3)
    stream[...] = arrived[2].astype(F32)
    begin(2)
    attention(2, lambda: forward_y(3, 2), lambda: forward_z(3, 2))

    begin(3)
    mlp()

    order = one_hot(lambda o: ((o // 64) * 4 + (o // 4) % 4) * 16 + (o % 4) * 4 + (o // 16) % 4)
    leaving[2] = dot(order, stream[...].astype(BF16)).astype(BF16)
    def keep3():
        arrived[3, rows(slot3 * 16, 16), :] = leaving[2, rows(f * 16, 16), :]

    send_all(copies3(), at_home, keep3)
    unless(at_home, 3, lambda copy: copy.wait_recv())
    order = one_hot(lambda o: (((o // 32) % 2) * 8 + o % 8) * 16 + (o // 64) * 4 + (o // 8) % 4)
    out_ref[...] = dot(order, arrived[3]).astype(BF16)

    t_total(0, 224).wait_send()
    t_total(1, 240).wait_send()
    unless(stays, 2, lambda copy: copy.wait_send())
    unless(at_home, 3, lambda copy: copy.wait_send())
    for p in range(4):
        for _ in range(3):
            w_total(p, 0, 0, 8).wait_send()
        share_copy(p).wait_send()
        return_copy(p).wait_send()


def local(tokens, norm_gain, qkv_weight, qk_gain, out_weight, ffn_in, ffn_out):
    qkv_src = qkv_weight.transpose(0, 2, 1, 3)
    in_src = ffn_in.transpose(1, 0, 2)
    vmem, hbm = pl.BlockSpec(memory_space=pltpu.VMEM), pl.BlockSpec(memory_space=pl.ANY)
    result = pl.pallas_call(
        kernel,
        out_shape=jax.ShapeDtypeStruct((ROWS, D), BF16),
        in_specs=[hbm, hbm, hbm, hbm, hbm, vmem, vmem],
        out_specs=vmem,
        scratch_shapes=[
            pltpu.VMEM((3, 4, 3, D, 128), BF16),
            pltpu.VMEM((3, 512, D), BF16),
            pltpu.VMEM((4, 2, D, 256), BF16),
            pltpu.VMEM((D, D), BF16),
            pltpu.VMEM((4, ROWS, D), BF16),
            pltpu.VMEM((3, ROWS, D), BF16),
            pltpu.VMEM((ROWS, D), F32),
            pltpu.VMEM((4, 2 * ROWS, D), BF16),
            pltpu.VMEM((4, ROWS, D), BF16),
            pltpu.VMEM((4, ROWS, D), BF16),
            pltpu.VMEM((2 * ROWS, 384), BF16),
            pltpu.VMEM((2 * ROWS, 512), BF16),
            pltpu.VMEM((2 * ROWS, D), BF16),
            pltpu.VMEM((ROWS, ROWS), BF16),
            pltpu.SemaphoreType.DMA((4,)),
            pltpu.SemaphoreType.DMA((4, 4, 3)),
            pltpu.SemaphoreType.DMA((5, 2)),
            pltpu.SemaphoreType.DMA((4,)),
            pltpu.SemaphoreType.DMA((4,)),
            pltpu.SemaphoreType.DMA((4, 2)),
            pltpu.SemaphoreType.DMA((4, 2)),
            pltpu.SemaphoreType.REGULAR((3,)),
        ],
        compiler_params=pltpu.CompilerParams(collective_id=0, has_side_effects=True, vmem_limit_bytes=60 * 2**20),
    )(tokens.reshape(ROWS, D), qkv_src, out_weight, in_src, ffn_out, norm_gain, qk_gain)
    return result.reshape(tokens.shape)


def solution(mesh):
    return jax.shard_map(
        local,
        mesh=mesh,
        in_specs=(
            P(None, "ta", "ha", "wa", None),
            P(),
            P(None, None, None, "ta"),
            P(),
            P(None, "ta", None),
            P(None, None, "ta"),
            P("ta", None),
        ),
        out_specs=P(None, "ta", "ha", "wa", None),
        check_vma=False,
    )
```

```python
import functools

import jax
import jax.numpy as jnp
from jax import lax
from jax.experimental import pallas as pl
from jax.experimental.pallas import tpu as pltpu
from jax.sharding import PartitionSpec as P

MESH = pl.DeviceIdType.MESH
BF16, F32 = jnp.bfloat16, jnp.float32
ROWS = 256
UNIT = 128
D = 1024


def place(x, y, z, k):
    return {"ta": x, "ha": (z // 2) * 2 + k, "wa": (z % 2) * 4 + y}


def rows(start, size):
    return pl.ds(pl.multiple_of(start, size), size)


def dot_t(a, b):
    return lax.dot_general(a, b, (((1,), (1,)), ((), ())), preferred_element_type=F32)


def dot(a, b):
    return jnp.dot(a, b, preferred_element_type=F32)


def rms(stream, gain_row):
    return stream * lax.rsqrt(jnp.mean(stream * stream, axis=-1, keepdims=True) + 1e-6) * gain_row


def iotas(shape):
    return lax.broadcasted_iota(jnp.int32, shape, 0), lax.broadcasted_iota(jnp.int32, shape, 1)


def one_hot(source_of):
    out, into = iotas((ROWS, ROWS))
    return jnp.where(source_of(out) == into, 1.0, 0.0).astype(BF16)


def kernel(
    tok,
    qkv_src,
    out_src,
    in_src,
    down_src,
    norm_gain,
    qk_gain,
    out_ref,
    w_attn,
    w_out,
    w_in,
    w_down,
    arrived,
    leaving,
    stream,
    normed,
    partial,
    partial_in,
    qkv,
    heads,
    hidden,
    mask,
    raw,
    w_send,
    w_recv,
    own_sem,
    t_send,
    t_recv,
    p_send,
    p_recv,
    hello,
):
    x = lax.axis_index("ta")
    h = lax.axis_index("ha")
    w = lax.axis_index("wa")
    z_hi, k, z_lo, y = h // 2, h % 2, w // 4, w % 4
    z = z_hi * 2 + z_lo
    partner = place(x, y, z, 1 - k)

    def both(p, d, start, size):
        if p < 3:
            return w_attn.at[p, d, :, pl.ds(start, size), :], w_out.at[p, d * 128 : d * 128 + 128, pl.ds(start, size)]
        return w_in.at[d, :, pl.ds(start, size), :], w_down.at[d * 256 : d * 256 + 256, pl.ds(start, size)]

    def both_src(p, start, size):
        if p < 3:
            return (
                qkv_src.at[p, :, pl.ds(start, size), rows(k * 128, 128)],
                out_src.at[p, rows(k * 128, 128), pl.ds(start, size)],
            )
        return (
            w_in.at[0, :, pl.ds(start, size), :],
            down_src.at[rows(k * 256, 256), pl.ds(start, size)],
        )

    def w_copies(p, d, kind, src, dst, device):
        return [
            pltpu.make_async_remote_copy(
                src_ref=a,
                dst_ref=b,
                send_sem=w_send.at[p],
                recv_sem=w_recv.at[p, d, kind],
                device_id=device,
                device_id_type=MESH,
            )
            for a, b in zip(src, dst)
        ]

    def w_total(p, d, kind, units):
        block = w_down.at[0 : (64 if p < 3 else 96) * units, :]
        return w_copies(p, d, kind, [block], [block], partner)[0]

    def w_wait(p, d, kind, units):
        w_total(p, d, kind, units).wait_recv()

    def unit(start):
        return pl.multiple_of(start, UNIT)

    gamma = pl.multiple_of(512 + z_lo * 256, 256)

    def start_all(copies):
        for copy in copies:
            copy.start()

    def x_send(p, kind):
        for e in (1, 3):
            start, size = ((unit(y * UNIT), UNIT), (gamma, 256))[kind]
            start_all(
                w_copies(p, 4 - e, kind, both_src(p, start, size), both(p, 4 - e, start, size), place((x + e) % 4, y, z, k))
            )

    def x_relay(p, d, kind, start):
        block, there = both(p, d, start, UNIT), both(p, 2, start, UNIT)
        start_all(w_copies(p, 2, kind, block, there, place((x + 4 - d) % 4, y, z, k)))

    def forward_y(p, *quarters):
        for d in quarters:
            w_wait(p, d, 0, 1)
            block = both(p, d, unit(y * UNIT), UNIT)
            if d != 2:
                pl.when(k == (0 if d == 3 else 1))(lambda: x_relay(p, d, 0, unit(y * UNIT)))
            for e, kind in ((1, 3), (3, 4)):
                start_all(w_copies(p, d, kind, block, block, place(x, (y + e) % 4, z, k)))

    def relay_y(p, *quarters):
        for d in quarters:
            for kind in (3, 4):
                w_wait(p, d, kind, 1)
            for core, at, to in ((0, (y + 3) % 4, (y + 1) % 4), (1, (y + 1) % 4, (y + 3) % 4)):

                def send(at=at, to=to):
                    block = both(p, d, unit(at * UNIT), UNIT)
                    start_all(w_copies(p, d, 2, block, block, place(x, to, z, k)))

                pl.when(k == core)(send)

    def forward_z(p, *quarters):
        for d in quarters:
            w_wait(p, d, 1, 2)
            if d != 2:
                x_relay(p, d, 1, unit(gamma if d == 3 else gamma + UNIT))
            for side, step in ((0, 1), (1, 7)):
                block = both(p, d, unit(gamma + side * UNIT), UNIT)
                start_all(w_copies(p, d, 2, block, block, place(x, y, (z + step) % 8, k)))

    def own_copy(p, i):
        src, dst = (both_src(p, 0, D)[i], both(p, 0, 0, D)[i]) if (p, i) != (3, 0) else (in_src.at[:, :, rows(k * 256, 256)], raw)
        return pltpu.make_async_copy(src, dst, own_sem.at[p, i])

    def split_in():
        own_copy(3, 0).wait()
        out, into = iotas((2 * UNIT, 2 * UNIT))
        pick = jnp.where(into == 2 * (out % UNIT) + out // UNIT, 1.0, 0.0).astype(BF16)
        for block in range(D // UNIT):
            r = slice(block * UNIT, block * UNIT + UNIT)
            apart = dot(pick, raw[r].reshape(2 * UNIT, 256)).astype(BF16)
            w_in[0, 0, r, :] = apart[:UNIT]
            w_in[0, 1, r, :] = apart[UNIT:]

    def own_in(p):
        if p < 3:
            own_copy(p, 0).wait()
        own_copy(p, 1).wait()

    def weights_in(p, d):
        w_wait(p, d, 2, 3)

    def t_copy(stage, src, dst, device):
        return pltpu.make_async_remote_copy(
            src_ref=src,
            dst_ref=dst,
            send_sem=t_send.at[stage],
            recv_sem=t_recv.at[stage],
            device_id=device,
            device_id_type=MESH,
        )

    def copies0():
        out = []
        for d in range(1, 8):
            to = (w + d) % 8
            start = (to % 4) * 64 + (to // 4) * 32
            out.append(
                t_copy(0, tok.at[rows(start, 32), :], arrived.at[0, rows(w * 32, 32), :], {"ta": x, "ha": h, "wa": to})
            )
        return out

    def t_total(stage, count):
        block = arrived.at[stage, 0:count, :]
        return t_copy(stage, block, block, partner)

    own_rows = pltpu.make_async_copy(
        tok.at[rows(y * 64 + z_lo * 32, 32), :], arrived.at[0, rows(w * 32, 32), :], own_sem.at[4, 0]
    )

    j = z * 2 + k
    group = z_hi * 4 + k * 2 + z_lo

    def copies1():
        out = []
        for d in range(1, 16):
            to = (j + d) % 16
            to_z, to_k = to // 2, to % 2
            block = (to_z % 2) * 8 + (to_z // 2) * 2 + to_k
            out.append(
                t_copy(
                    1, leaving.at[0, rows(block * 16, 16), :], arrived.at[1, rows(group * 16, 16), :], place(x, y, to_z, to_k)
                )
            )
        return out

    f = x * 4 + y

    def turn(to_y):
        return (to_y + 2 * z_lo + k) % 4

    def moved(c, to_x):
        half_way = jnp.where(c == 2, jnp.where(to_x // 2 == 0, 1, 3), jnp.where(to_x % 2 == 0, c, 0))
        return jnp.where(c == 0, 0, half_way)

    def copies2():
        out = []
        for d in range(16):
            to = (f + d) % 16
            to_x, to_y = to // 4, to % 4
            c = turn(to_y)
            block = ((z_hi + c) % 4) * 4 + to_x
            to_z = ((z_hi + moved(c, to_x)) % 4) * 2 + z_lo
            copy = t_copy(2, leaving.at[1, rows(block * 16, 16), :], arrived.at[2, rows(f * 16, 16), :], place(to_x, to_y, to_z, k))
            out.append((d == 0, copy))
        return out

    my_turn = turn(y)
    stays = moved(my_turn, x) == 0
    from_hi = (z_hi + 4 - moved(my_turn, x)) % 4

    slot3 = (x % 2) * 8 + from_hi * 2 + k
    to_hi = (from_hi + my_turn) % 4
    at_home = jnp.logical_and(z_hi == to_hi, k == x // 2)

    def copies3():
        out = []
        for dx in range(4):
            for dy in range(4):
                to_x, to_y = (x + dx) % 4, (y + dy) % 4
                copy = t_copy(
                    3,
                    leaving.at[2, rows((to_x * 4 + to_y) * 16, 16), :],
                    arrived.at[3, rows(slot3 * 16, 16), :],
                    place(to_x, to_y, to_hi * 2 + z_lo, x // 2),
                )
                out.append((dx == 0 and dy == 0, copy))
        return out

    def unless(kept, stage, act):
        pl.when(kept)(lambda: act(t_total(stage, 240)))
        pl.when(jnp.logical_not(kept))(lambda: act(t_total(stage, 256)))

    def send_all(copies, kept, keep):
        for maybe_self, copy in copies:
            if maybe_self:
                pl.when(jnp.logical_not(kept))(copy.start)
                pl.when(kept)(keep)
            else:
                copy.start()

    def pair_copy(p, index, src, dst):
        return pltpu.make_async_remote_copy(
            src_ref=src,
            dst_ref=dst,
            send_sem=p_send.at[p, index],
            recv_sem=p_recv.at[p, index],
            device_id=partner,
            device_id_type=MESH,
        )

    def share_copy(p):
        return pair_copy(p, 0, normed.at[p, 0:ROWS, :], normed.at[p, ROWS : 2 * ROWS, :])

    def return_copy(p):
        return pair_copy(p, 1, partial.at[p], partial_in.at[p])

    def greet(stage, peers):
        for peer in peers:
            pl.semaphore_signal(hello.at[stage], inc=1, device_id=peer, device_id_type=MESH)

    lane = lax.broadcasted_iota(jnp.int32, (1, 128), 1)
    left = lane < 64

    own, other, all_rows = slice(0, ROWS), slice(ROWS, 2 * ROWS), slice(0, 2 * ROWS)

    def project(p, d, r):
        tokens = normed[p, r, :]
        both_heads = dot(tokens, jnp.concatenate([w_attn[p, d, 0], w_attn[p, d, 1]], axis=1))
        a, b = iotas((256, 256))
        gain = jnp.concatenate([qk_gain[p, 0:1, :] * 0.125] * 2 + [qk_gain[p, 1:2, :]] * 2, axis=1)
        sums = jnp.where(a // 64 == b // 64, 1.0 / 64.0, 0.0).astype(BF16)
        mean = dot((both_heads * both_heads).astype(BF16), sums)
        qkv[r, 256:384] = dot(tokens, w_attn[p, d, 2]).astype(BF16)
        qkv[r, 0:256] = (both_heads * lax.rsqrt(mean + 1e-6) * gain).astype(BF16)

    def attend(d, r):
        queries, key_rows = qkv[r, 0:128], qkv[r, 128:256]
        values = jnp.concatenate([qkv[r, 256:384], jnp.ones((ROWS, 128), BF16)], axis=1)
        results = []
        for side in range(2):
            mine = jnp.where(left if side == 0 else jnp.logical_not(left), queries, jnp.zeros_like(queries))
            weights = jnp.exp(dot_t(mine, key_rows)).astype(BF16) * mask[...]
            summed = dot(weights, values)
            results.append(summed[:, :128] / summed[:, 128:])
        heads[r, d * 128 : d * 128 + 128] = jnp.where(left, results[0], results[1]).astype(BF16)

    def attention(p, relay0=None, relay1=None, relay3=None):
        own_in(p)
        project(p, 0, own)
        attend(0, own)
        share_copy(p).wait_recv()
        project(p, 0, other)
        attend(0, other)
        for relay, d in ((relay0, 1), (relay1, 3)):
            if relay is not None:
                relay()
            weights_in(p, d)
            project(p, d, all_rows)
            attend(d, own)
            attend(d, other)
        if relay3 is not None:
            relay3()
        weights_in(p, 2)
        project(p, 2, other)
        attend(2, other)
        partial[p] = dot(heads[other, :], w_out[p]).astype(BF16)
        return_copy(p).start()
        project(p, 2, own)
        attend(2, own)
        finish(p, heads, w_out[p])

    def mlp_quarter(d, r):
        tokens = normed[3, r, :]
        gate = dot(tokens, w_in[d, 0])
        up = dot(tokens, w_in[d, 1])
        hidden[r, d * 256 : d * 256 + 256] = (gate / (1.0 + jnp.exp(-gate)) * up).astype(BF16)

    def mlp():
        own_in(3)
        mlp_quarter(0, own)
        share_copy(3).wait_recv()
        mlp_quarter(0, other)
        for d in (1, 3):
            weights_in(3, d)
            mlp_quarter(d, all_rows)
        weights_in(3, 2)
        mlp_quarter(2, other)
        partial[3] = dot(hidden[other, :], w_down[...]).astype(BF16)
        return_copy(3).start()
        mlp_quarter(2, own)
        finish(3, hidden, w_down[...])

    def finish(p, left_ref, right_ref):
        stream[...] = stream[...] + dot(left_ref[own, :], right_ref)
        return_copy(p).wait_recv()
        stream[...] = stream[...] + partial_in[p].astype(F32)

    def begin(p):
        normed[p, 0:ROWS, :] = rms(stream[...], norm_gain[p : p + 1, :]).astype(BF16)
        share_copy(p).start()

    for p in range(4):
        own_copy(p, 0).start()
        own_copy(p, 1).start()
    own_rows.start()
    barrier = pltpu.get_barrier_semaphore()
    greeted = [place((x + e) % 4, y, z, k) for e in (1, 2, 3)]
    greeted += [{"ta": x, "ha": h, "wa": (w + d) % 8} for d in range(1, 8)]
    greeted += [partner, place(x, y, (z + 7 + 2 * z_lo) % 8, k)]
    for peer in greeted:
        pl.semaphore_signal(barrier, inc=1, device_id=peer, device_id_type=MESH)
    pl.semaphore_wait(barrier, len(greeted))
    start_all(copies0())
    x_send(0, 0)
    x_send(0, 1)
    greet(0, [place(x, y, (z + 1) % 8, k), place(x, y, (z + 7) % 8, k)])

    a, b = iotas((ROWS, ROWS))
    mask[...] = jnp.where((a // 8) % 4 == (b // 8) % 4, 1.0, 0.0).astype(BF16)
    pl.semaphore_wait(hello.at[0], 2)
    greet(1, [place(x, y, (z + 2) % 8, k), place(x, y, (z + 6) % 8, k)])
    forward_y(0, 1, 3)
    x_send(1, 0)
    own_rows.wait()
    t_total(0, 224).wait_recv()
    stream[...] = arrived[0].astype(F32)
    begin(0)
    pl.semaphore_wait(hello.at[1], 2)
    greet(2, [partner])

    def relays00():
        forward_z(0, 1, 3)
        x_send(1, 1)
        relay_y(0, 1)
        forward_y(0, 2)
        relay_y(0, 3)
        split_in()

    def relays01():
        forward_z(0, 2)
        relay_y(0, 2)
        forward_y(1, 1, 3)
        x_send(2, 0)

    def relays02():
        forward_z(1, 1, 3)
        x_send(2, 1)

    attention(0, relays00, relays01, relays02)
    pl.semaphore_wait(hello.at[2], 1)

    order = one_hot(lambda o: ((o // 128) * 4 + o % 4) * 32 + ((o // 4) % 4) * 8 + (o // 16) % 8)
    leaving[0] = dot(order, stream[...].astype(BF16)).astype(BF16)
    start_all(copies1())
    own_block = z_lo * 8 + z_hi * 2 + k
    arrived[1, rows(group * 16, 16), :] = leaving[0, rows(own_block * 16, 16), :]
    a, b = iotas((ROWS, ROWS))
    mask[...] = jnp.where(a % 4 == b % 4, 1.0, 0.0).astype(BF16)
    relay_y(1, 1, 3)
    forward_y(1, 2)
    forward_z(1, 2)
    forward_y(2, 1, 3)
    x_send(3, 0)
    relay_y(1, 2)
    t_total(1, 240).wait_recv()
    stream[...] = arrived[1].astype(F32)
    begin(1)
    forward_z(2, 1, 3)
    x_send(3, 1)
    relay_y(2, 1, 3)
    forward_y(2, 2)

    def relays12():
        forward_y(3, 1, 3)
        forward_z(2, 2)

    attention(1, None, None, relays12)

    leaving[1] = stream[...].astype(BF16)

    def keep2():
        arrived[2, rows(f * 16, 16), :] = leaving[1, rows((((z_hi + my_turn) % 4) * 4 + x) * 16, 16), :]

    send_all(copies2(), stays, keep2)
    a, b = iotas((ROWS, ROWS))
    mask[...] = jnp.where(jnp.logical_and(a % 16 == b % 16, b // 16 <= a // 16), 1.0, 0.0).astype(BF16)
    relay_y(2, 2)
    unless(stays, 2, lambda copy: copy.wait_recv())
    forward_y(3, 2)
    forward_z(3, 1, 3)
    relay_y(3, 1, 3)
    stream[...] = arrived[2].astype(F32)
    begin(2)

    def relays21():
        forward_z(3, 2)
        relay_y(3, 2)

    attention(2, None, None, relays21)

    begin(3)
    mlp()

    order = one_hot(lambda o: ((o // 64) * 4 + (o // 4) % 4) * 16 + (o % 4) * 4 + (o // 16) % 4)
    leaving[2] = dot(order, stream[...].astype(BF16)).astype(BF16)
    def keep3():
        arrived[3, rows(slot3 * 16, 16), :] = leaving[2, rows(f * 16, 16), :]

    send_all(copies3(), at_home, keep3)
    unless(at_home, 3, lambda copy: copy.wait_recv())
    order = one_hot(lambda o: (((o // 32) % 2) * 8 + o % 8) * 16 + (o // 64) * 4 + (o // 8) % 4)
    out_ref[...] = dot(order, arrived[3]).astype(BF16)

    t_total(0, 224).wait_send()
    t_total(1, 240).wait_send()
    unless(stays, 2, lambda copy: copy.wait_send())
    unless(at_home, 3, lambda copy: copy.wait_send())
    for p in range(4):
        for _ in range(3):
            w_total(p, 0, 0, 8).wait_send()
        share_copy(p).wait_send()
        return_copy(p).wait_send()


def local(tokens, norm_gain, qkv_weight, qk_gain, out_weight, ffn_in, ffn_out):
    qkv_src = qkv_weight.transpose(0, 2, 1, 3)
    vmem, hbm = pl.BlockSpec(memory_space=pltpu.VMEM), pl.BlockSpec(memory_space=pl.ANY)
    result = pl.pallas_call(
        kernel,
        out_shape=jax.ShapeDtypeStruct((ROWS, D), BF16),
        in_specs=[hbm, hbm, hbm, hbm, hbm, vmem, vmem],
        out_specs=vmem,
        scratch_shapes=[
            pltpu.VMEM((3, 4, 3, D, 128), BF16),
            pltpu.VMEM((3, 512, D), BF16),
            pltpu.VMEM((4, 2, D, 256), BF16),
            pltpu.VMEM((D, D), BF16),
            pltpu.VMEM((4, ROWS, D), BF16),
            pltpu.VMEM((3, ROWS, D), BF16),
            pltpu.VMEM((ROWS, D), F32),
            pltpu.VMEM((4, 2 * ROWS, D), BF16),
            pltpu.VMEM((4, ROWS, D), BF16),
            pltpu.VMEM((4, ROWS, D), BF16),
            pltpu.VMEM((2 * ROWS, 384), BF16),
            pltpu.VMEM((2 * ROWS, 512), BF16),
            pltpu.VMEM((2 * ROWS, D), BF16),
            pltpu.VMEM((ROWS, ROWS), BF16),
            pltpu.VMEM((D, 2, 256), BF16),
            pltpu.SemaphoreType.DMA((4,)),
            pltpu.SemaphoreType.DMA((4, 4, 5)),
            pltpu.SemaphoreType.DMA((5, 2)),
            pltpu.SemaphoreType.DMA((4,)),
            pltpu.SemaphoreType.DMA((4,)),
            pltpu.SemaphoreType.DMA((4, 2)),
            pltpu.SemaphoreType.DMA((4, 2)),
            pltpu.SemaphoreType.REGULAR((3,)),
        ],
        compiler_params=pltpu.CompilerParams(collective_id=0, has_side_effects=True, vmem_limit_bytes=60 * 2**20),
    )(tokens.reshape(ROWS, D), qkv_src, out_weight, ffn_in, ffn_out, norm_gain, qk_gain)
    return result.reshape(tokens.shape)


def solution(mesh):
    return jax.shard_map(
        local,
        mesh=mesh,
        in_specs=(
            P(None, "ta", "ha", "wa", None),
            P(),
            P(None, None, None, "ta"),
            P(),
            P(None, "ta", None),
            P(None, None, "ta"),
            P("ta", None),
        ),
        out_specs=P(None, "ta", "ha", "wa", None),
        check_vma=False,
    )
```

```python
import functools

import jax
import jax.numpy as jnp
from jax import lax
from jax.experimental import pallas as pl
from jax.experimental.pallas import tpu as pltpu
from jax.sharding import PartitionSpec as P

MESH = pl.DeviceIdType.MESH
BF16, F32 = jnp.bfloat16, jnp.float32
ROWS = 256
UNIT = 128
D = 1024


def place(x, y, z, k):
    return {"ta": x, "ha": (z // 2) * 2 + k, "wa": (z % 2) * 4 + y}


def rows(start, size):
    return pl.ds(pl.multiple_of(start, size), size)


def dot_t(a, b):
    return lax.dot_general(a, b, (((1,), (1,)), ((), ())), preferred_element_type=F32)


def dot(a, b):
    return jnp.dot(a, b, preferred_element_type=F32)


def rms(stream, gain_row):
    return stream * lax.rsqrt(jnp.mean(stream * stream, axis=-1, keepdims=True) + 1e-6) * gain_row


def iotas(shape):
    return lax.broadcasted_iota(jnp.int32, shape, 0), lax.broadcasted_iota(jnp.int32, shape, 1)


def one_hot(source_of):
    out, into = iotas((ROWS, ROWS))
    return jnp.where(source_of(out) == into, 1.0, 0.0).astype(BF16)


def kernel(
    tok,
    qkv_src,
    out_src,
    in_src,
    down_src,
    norm_gain,
    qk_gain,
    out_ref,
    w_attn,
    w_out,
    w_in,
    w_down,
    arrived,
    leaving,
    stream,
    normed,
    partial,
    partial_in,
    qkv,
    heads,
    hidden,
    mask,
    raw,
    tok_in,
    w_send,
    w_recv,
    own_sem,
    t_send,
    t_recv,
    p_send,
    p_recv,
    hello,
):
    x = lax.axis_index("ta")
    h = lax.axis_index("ha")
    w = lax.axis_index("wa")
    z_hi, k, z_lo, y = h // 2, h % 2, w // 4, w % 4
    z = z_hi * 2 + z_lo
    partner = place(x, y, z, 1 - k)

    def both(p, d, start, size):
        if p < 3:
            return w_attn.at[p, d, pl.ds(start, size), :], w_out.at[p, d * 128 : d * 128 + 128, pl.ds(start, size)]
        return w_in.at[d, :, pl.ds(start, size), :], w_down.at[d * 256 : d * 256 + 256, pl.ds(start, size)]

    def w_copies(p, d, kind, src, dst, device):
        return [
            pltpu.make_async_remote_copy(
                src_ref=a,
                dst_ref=b,
                send_sem=w_send.at[p],
                recv_sem=w_recv.at[p, d, kind],
                device_id=device,
                device_id_type=MESH,
            )
            for a, b in zip(src, dst)
        ]

    def w_total(p, d, kind, units):
        block = w_down.at[0 : (64 if p < 3 else 96) * units, :]
        return w_copies(p, d, kind, [block], [block], partner)[0]

    def w_wait(p, d, kind, units):
        w_total(p, d, kind, units).wait_recv()

    def unit(start):
        return pl.multiple_of(start, UNIT)

    gamma = pl.multiple_of(512 + z_lo * 256, 256)

    def start_all(copies):
        for copy in copies:
            copy.start()

    def x_send(p, kind):
        for e in (1, 3):
            start, size = ((unit(y * UNIT), UNIT), (gamma, 256))[kind]
            start_all(
                w_copies(p, 4 - e, kind, both(p, 0, start, size), both(p, 4 - e, start, size), place((x + e) % 4, y, z, k))
            )

    def x_relay(p, d, kind, start):
        block, there = both(p, d, start, UNIT), both(p, 2, start, UNIT)
        start_all(w_copies(p, 2, kind, block, there, place((x + 4 - d) % 4, y, z, k)))

    def forward_y(p, *quarters):
        for d in quarters:
            w_wait(p, d, 0, 1)
            block = both(p, d, unit(y * UNIT), UNIT)
            if d != 2:
                pl.when(k == (0 if d == 3 else 1))(lambda: x_relay(p, d, 0, unit(y * UNIT)))
            for e, kind in ((1, 3), (3, 4)):
                start_all(w_copies(p, d, kind, block, block, place(x, (y + e) % 4, z, k)))

    def relay_y(p, *quarters):
        for d in quarters:
            for kind in (3, 4):
                w_wait(p, d, kind, 1)
            for core, at, to in ((0, (y + 3) % 4, (y + 1) % 4), (1, (y + 1) % 4, (y + 3) % 4)):

                def send(at=at, to=to):
                    block = both(p, d, unit(at * UNIT), UNIT)
                    start_all(w_copies(p, d, 2, block, block, place(x, to, z, k)))

                pl.when(k == core)(send)

    def forward_z(p, *quarters):
        for d in quarters:
            w_wait(p, d, 1, 2)
            if d != 2:
                x_relay(p, d, 1, unit(gamma if d == 3 else gamma + UNIT))
            for side, step in ((0, 1), (1, 7)):
                block = both(p, d, unit(gamma + side * UNIT), UNIT)
                start_all(w_copies(p, d, 2, block, block, place(x, y, (z + step) % 8, k)))

    def own_copies(p):
        if p < 3:
            pairs = [(qkv_src.at[p, t, :, rows(k * 128, 128)], w_attn.at[p, 0, :, t * 128 : t * 128 + 128]) for t in range(3)]
            pairs.append((out_src.at[p, rows(k * 128, 128), :], w_out.at[p, 0:128, :]))
        else:
            pairs = [(in_src.at[:, :, rows(k * 256, 256)], raw), (down_src.at[rows(k * 256, 256), :], w_down.at[0:256, :])]
        return [pltpu.make_async_copy(a, b, own_sem.at[p, i]) for i, (a, b) in enumerate(pairs)]

    def split_in():
        own_in(3)
        out, into = iotas((2 * UNIT, 2 * UNIT))
        pick = jnp.where(into == 2 * (out % UNIT) + out // UNIT, 1.0, 0.0).astype(BF16)
        for block in range(D // UNIT):
            r = slice(block * UNIT, block * UNIT + UNIT)
            apart = dot(pick, raw[r].reshape(2 * UNIT, 256)).astype(BF16)
            w_in[0, 0, r, :] = apart[:UNIT]
            w_in[0, 1, r, :] = apart[UNIT:]

    def own_in(p):
        for copy in own_copies(p):
            copy.wait()

    def weights_in(p, d):
        w_wait(p, d, 2, 3)

    def t_copy(stage, src, dst, device):
        return pltpu.make_async_remote_copy(
            src_ref=src,
            dst_ref=dst,
            send_sem=t_send.at[stage],
            recv_sem=t_recv.at[stage],
            device_id=device,
            device_id_type=MESH,
        )

    def copies0():
        out = []
        for d in range(1, 8):
            to = (w + d) % 8
            start = (to % 4) * 64 + (to // 4) * 32
            out.append(
                t_copy(0, tok_in.at[rows(start, 32), :], arrived.at[0, rows(w * 32, 32), :], {"ta": x, "ha": h, "wa": to})
            )
        return out

    def t_total(stage, count):
        block = arrived.at[stage, 0:count, :]
        return t_copy(stage, block, block, partner)

    tokens_in = pltpu.make_async_copy(tok, tok_in, own_sem.at[4, 0])

    j = z * 2 + k
    group = z_hi * 4 + k * 2 + z_lo

    def copies1(cols):
        out = []
        for d in range(1, 16):
            to = (j + d) % 16
            to_z, to_k = to // 2, to % 2
            block = (to_z % 2) * 8 + (to_z // 2) * 2 + to_k
            out.append(
                t_copy(
                    1, leaving.at[0, rows(block * 16, 16), cols], arrived.at[1, rows(group * 16, 16), cols], place(x, y, to_z, to_k)
                )
            )
        return out

    f = x * 4 + y

    def turn(to_y):
        return (to_y + 2 * z_lo + k) % 4

    def moved(c, to_x):
        half_way = jnp.where(c == 2, jnp.where(to_x // 2 == 0, 1, 3), jnp.where(to_x % 2 == 0, c, 0))
        return jnp.where(c == 0, 0, half_way)

    def copies2(cols):
        out = []
        for d in range(16):
            to = (f + d) % 16
            to_x, to_y = to // 4, to % 4
            c = turn(to_y)
            block = ((z_hi + c) % 4) * 4 + to_x
            to_z = ((z_hi + moved(c, to_x)) % 4) * 2 + z_lo
            copy = t_copy(2, leaving.at[1, rows(block * 16, 16), cols], arrived.at[2, rows(f * 16, 16), cols], place(to_x, to_y, to_z, k))
            out.append((d == 0, copy))
        return out

    my_turn = turn(y)
    stays = moved(my_turn, x) == 0
    from_hi = (z_hi + 4 - moved(my_turn, x)) % 4

    slot3 = (x % 2) * 8 + from_hi * 2 + k
    to_hi = (from_hi + my_turn) % 4
    at_home = jnp.logical_and(z_hi == to_hi, k == x // 2)

    def copies3(cols):
        out = []
        for dx in range(4):
            for dy in range(4):
                to_x, to_y = (x + dx) % 4, (y + dy) % 4
                copy = t_copy(
                    3,
                    leaving.at[2, rows((to_x * 4 + to_y) * 16, 16), cols],
                    arrived.at[3, rows(slot3 * 16, 16), cols],
                    place(to_x, to_y, to_hi * 2 + z_lo, x // 2),
                )
                out.append((dx == 0 and dy == 0, copy))
        return out

    def unless(kept, stage, act):
        pl.when(kept)(lambda: act(t_total(stage, 240)))
        pl.when(jnp.logical_not(kept))(lambda: act(t_total(stage, 256)))

    def send_all(copies, kept):
        for maybe_self, copy in copies:
            if maybe_self:
                pl.when(jnp.logical_not(kept))(copy.start)
            else:
                copy.start()

    def keep2():
        arrived[2, rows(f * 16, 16), :] = leaving[1, rows((((z_hi + my_turn) % 4) * 4 + x) * 16, 16), :]

    def keep3():
        arrived[3, rows(slot3 * 16, 16), :] = leaving[2, rows(f * 16, 16), :]

    def leave1(cols):
        order = one_hot(lambda o: ((o // 128) * 4 + o % 4) * 32 + ((o // 4) % 4) * 8 + (o // 16) % 8)
        leaving[0, :, cols] = dot(order, stream[:, cols].astype(BF16)).astype(BF16)
        if cols.start == 0:
            pl.semaphore_wait(hello.at[2], 1)
        start_all(copies1(cols))

    def leave2(cols):
        leaving[1, :, cols] = stream[:, cols].astype(BF16)
        send_all(copies2(cols), stays)

    def leave3(cols):
        order = one_hot(lambda o: ((o // 64) * 4 + (o // 4) % 4) * 16 + (o % 4) * 4 + (o // 16) % 4)
        leaving[2, :, cols] = dot(order, stream[:, cols].astype(BF16)).astype(BF16)
        send_all(copies3(cols), at_home)

    def pair_copy(p, index, src, dst):
        return pltpu.make_async_remote_copy(
            src_ref=src,
            dst_ref=dst,
            send_sem=p_send.at[p, index],
            recv_sem=p_recv.at[p, index],
            device_id=partner,
            device_id_type=MESH,
        )

    def share_copy(p):
        return pair_copy(p, 0, normed.at[p, 0:ROWS, :], normed.at[p, ROWS : 2 * ROWS, :])

    halves = (slice(0, D // 2), slice(D // 2, D))

    def return_copy(p, half):
        return pair_copy(p, 1 + half, partial.at[p, :, halves[half]], partial_in.at[p, :, halves[half]])

    def greet(stage, peers):
        for peer in peers:
            pl.semaphore_signal(hello.at[stage], inc=1, device_id=peer, device_id_type=MESH)

    lane = lax.broadcasted_iota(jnp.int32, (1, 128), 1)
    left = lane < 64

    own, other, all_rows = slice(0, ROWS), slice(ROWS, 2 * ROWS), slice(0, 2 * ROWS)

    def project(p, d, r):
        tokens = normed[p, r, :]
        both_heads = dot(tokens, w_attn[p, d, :, 0:256])
        a, b = iotas((256, 256))
        gain = jnp.concatenate([qk_gain[p, 0:1, :] * 0.125] * 2 + [qk_gain[p, 1:2, :]] * 2, axis=1)
        sums = jnp.where(a // 64 == b // 64, 1.0 / 64.0, 0.0).astype(BF16)
        mean = dot((both_heads * both_heads).astype(BF16), sums)
        qkv[r, 256:384] = dot(tokens, w_attn[p, d, :, 256:384]).astype(BF16)
        qkv[r, 0:256] = (both_heads * lax.rsqrt(mean + 1e-6) * gain).astype(BF16)

    def attend(d, r):
        queries, key_rows = qkv[r, 0:128], qkv[r, 128:256]
        values = jnp.concatenate([qkv[r, 256:384], jnp.ones((ROWS, 128), BF16)], axis=1)
        results = []
        for side in range(2):
            mine = jnp.where(left if side == 0 else jnp.logical_not(left), queries, jnp.zeros_like(queries))
            weights = jnp.exp(dot_t(mine, key_rows)).astype(BF16) * mask[...]
            summed = dot(weights, values)
            results.append(summed[:, :128] / summed[:, 128:])
        heads[r, d * 128 : d * 128 + 128] = jnp.where(left, results[0], results[1]).astype(BF16)

    def attention(p, after, relay0=None, relay1=None, relay3=None):
        project(p, 0, own)
        attend(0, own)
        share_copy(p).wait_recv()
        project(p, 0, other)
        attend(0, other)
        for relay, d in ((relay0, 1), (relay1, 3)):
            if relay is not None:
                relay()
            weights_in(p, d)
            project(p, d, all_rows)
            attend(d, own)
            attend(d, other)
        if relay3 is not None:
            relay3()
        weights_in(p, 2)
        project(p, 2, other)
        attend(2, other)
        give(p, heads, w_out.at[p])
        project(p, 2, own)
        attend(2, own)
        finish(p, heads, w_out.at[p], after)

    def mlp_quarter(d, r):
        tokens = normed[3, r, :]
        gate = dot(tokens, w_in[d, 0])
        up = dot(tokens, w_in[d, 1])
        hidden[r, d * 256 : d * 256 + 256] = (gate / (1.0 + jnp.exp(-gate)) * up).astype(BF16)

    def mlp(after):
        weights_in(3, 1)
        for d in (0, 1):
            mlp_quarter(d, own)
        share_copy(3).wait_recv()
        for d in (0, 1):
            mlp_quarter(d, other)
        weights_in(3, 3)
        mlp_quarter(3, all_rows)
        weights_in(3, 2)
        mlp_quarter(2, other)
        give(3, hidden, w_down)
        mlp_quarter(2, own)
        finish(3, hidden, w_down, after)

    def give(p, left_ref, right_ref):
        for half, cols in enumerate(halves):
            partial[p, :, cols] = dot(left_ref[other, :], right_ref[:, cols]).astype(BF16)
            return_copy(p, half).start()

    def finish(p, left_ref, right_ref, after):
        for half, cols in enumerate(halves):
            summed = stream[:, cols] + dot(left_ref[own, :], right_ref[:, cols])
            return_copy(p, half).wait_recv()
            stream[:, cols] = summed + partial_in[p, :, cols].astype(F32)
            after(cols)

    def begin(p):
        normed[p, 0:ROWS, :] = rms(stream[...], norm_gain[p : p + 1, :]).astype(BF16)
        share_copy(p).start()

    tokens_in.start()
    for p in range(4):
        start_all(own_copies(p))
    barrier = pltpu.get_barrier_semaphore()
    greeted = [place((x + e) % 4, y, z, k) for e in (1, 2, 3)]
    greeted += [{"ta": x, "ha": h, "wa": (w + d) % 8} for d in range(1, 8)]
    greeted += [partner, place(x, y, (z + 7 + 2 * z_lo) % 8, k)]
    for peer in greeted:
        pl.semaphore_signal(barrier, inc=1, device_id=peer, device_id_type=MESH)
    pl.semaphore_wait(barrier, len(greeted))
    tokens_in.wait()
    start_all(copies0())
    own_in(0)
    x_send(0, 0)
    x_send(0, 1)
    greet(0, [place(x, y, (z + 1) % 8, k), place(x, y, (z + 7) % 8, k)])
    own_in(1)
    own_in(2)
    arrived[0, rows(w * 32, 32), :] = tok_in[rows(y * 64 + z_lo * 32, 32), :]

    a, b = iotas((ROWS, ROWS))
    mask[...] = jnp.where((a // 8) % 4 == (b // 8) % 4, 1.0, 0.0).astype(BF16)
    pl.semaphore_wait(hello.at[0], 2)
    greet(1, [place(x, y, (z + 2) % 8, k), place(x, y, (z + 6) % 8, k)])
    forward_y(0, 1, 3)
    x_send(1, 0)
    t_total(0, 224).wait_recv()
    stream[...] = arrived[0].astype(F32)
    begin(0)
    pl.semaphore_wait(hello.at[1], 2)
    greet(2, [partner])

    def relays00():
        forward_z(0, 1, 3)
        x_send(1, 1)
        relay_y(0, 1)
        forward_y(0, 2)
        relay_y(0, 3)
        split_in()
        relay_y(0, 2)
        forward_z(0, 2)

    def relays01():
        forward_y(1, 1, 3)
        x_send(2, 0)

    def relays02():
        forward_z(1, 1, 3)
        x_send(2, 1)

    attention(0, leave1, relays00, relays01, relays02)

    own_block = z_lo * 8 + z_hi * 2 + k
    arrived[1, rows(group * 16, 16), :] = leaving[0, rows(own_block * 16, 16), :]
    a, b = iotas((ROWS, ROWS))
    mask[...] = jnp.where(a % 4 == b % 4, 1.0, 0.0).astype(BF16)
    relay_y(1, 1, 3)
    forward_y(1, 2)
    forward_z(1, 2)
    forward_y(2, 1, 3)
    x_send(3, 0)
    relay_y(1, 2)
    t_total(1, 240).wait_recv()
    stream[...] = arrived[1].astype(F32)
    begin(1)
    forward_z(2, 1, 3)
    x_send(3, 1)
    relay_y(2, 1, 3)
    forward_y(2, 2)

    def relays12():
        forward_y(3, 1, 3)
        forward_z(2, 2)

    attention(1, leave2, None, None, relays12)

    pl.when(stays)(keep2)
    a, b = iotas((ROWS, ROWS))
    mask[...] = jnp.where(jnp.logical_and(a % 16 == b % 16, b // 16 <= a // 16), 1.0, 0.0).astype(BF16)
    relay_y(2, 2)
    unless(stays, 2, lambda copy: copy.wait_recv())
    forward_y(3, 2)
    forward_z(3, 1, 3)
    relay_y(3, 1, 3)
    stream[...] = arrived[2].astype(F32)
    begin(2)

    def relays21():
        forward_z(3, 2)
        relay_y(3, 2)

    attention(2, lambda cols: None, None, None, relays21)

    begin(3)
    mlp(leave3)

    pl.when(at_home)(keep3)
    unless(at_home, 3, lambda copy: copy.wait_recv())
    order = one_hot(lambda o: (((o // 32) % 2) * 8 + o % 8) * 16 + (o // 64) * 4 + (o // 8) % 4)
    out_ref[...] = dot(order, arrived[3]).astype(BF16)

    t_total(0, 224).wait_send()
    t_total(1, 240).wait_send()
    unless(stays, 2, lambda copy: copy.wait_send())
    unless(at_home, 3, lambda copy: copy.wait_send())
    for p in range(4):
        for _ in range(3):
            w_total(p, 0, 0, 8).wait_send()
        share_copy(p).wait_send()
        return_copy(p, 0).wait_send()
        return_copy(p, 1).wait_send()


def local(tokens, norm_gain, qkv_weight, qk_gain, out_weight, ffn_in, ffn_out):
    qkv_src = qkv_weight.transpose(0, 2, 1, 3)
    vmem, hbm = pl.BlockSpec(memory_space=pltpu.VMEM), pl.BlockSpec(memory_space=pl.ANY)
    result = pl.pallas_call(
        kernel,
        out_shape=pltpu.VMEM((ROWS, D), BF16),
        in_specs=[hbm, hbm, hbm, hbm, hbm, vmem, vmem],
        out_specs=vmem,
        scratch_shapes=[
            pltpu.VMEM((3, 4, D, 384), BF16),
            pltpu.VMEM((3, 512, D), BF16),
            pltpu.VMEM((4, 2, D, 256), BF16),
            pltpu.VMEM((D, D), BF16),
            pltpu.VMEM((4, ROWS, D), BF16),
            pltpu.VMEM((3, ROWS, D), BF16),
            pltpu.VMEM((ROWS, D), F32),
            pltpu.VMEM((4, 2 * ROWS, D), BF16),
            pltpu.VMEM((4, ROWS, D), BF16),
            pltpu.VMEM((4, ROWS, D), BF16),
            pltpu.VMEM((2 * ROWS, 384), BF16),
            pltpu.VMEM((2 * ROWS, 512), BF16),
            pltpu.VMEM((2 * ROWS, D), BF16),
            pltpu.VMEM((ROWS, ROWS), BF16),
            pltpu.VMEM((D, 2, 256), BF16),
            pltpu.VMEM((ROWS, D), BF16),
            pltpu.SemaphoreType.DMA((4,)),
            pltpu.SemaphoreType.DMA((4, 4, 5)),
            pltpu.SemaphoreType.DMA((5, 4)),
            pltpu.SemaphoreType.DMA((4,)),
            pltpu.SemaphoreType.DMA((4,)),
            pltpu.SemaphoreType.DMA((4, 3)),
            pltpu.SemaphoreType.DMA((4, 3)),
            pltpu.SemaphoreType.REGULAR((3,)),
        ],
        compiler_params=pltpu.CompilerParams(collective_id=0, has_side_effects=True, vmem_limit_bytes=60 * 2**20),
    )(tokens.reshape(ROWS, D), qkv_src, out_weight, ffn_in, ffn_out, norm_gain, qk_gain)
    return result.reshape(tokens.shape)


def solution(mesh):
    return jax.shard_map(
        local,
        mesh=mesh,
        in_specs=(
            P(None, "ta", "ha", "wa", None),
            P(),
            P(None, None, None, "ta"),
            P(),
            P(None, "ta", None),
            P(None, None, "ta"),
            P("ta", None),
        ),
        out_specs=P(None, "ta", "ha", "wa", None),
        check_vma=False,
    )
```
